32 devices in a mesh: shot: 4 (over y, core), space: 8 (over z, x).
Axes of the slice: x: 2, y: 2, z: 4, core: 2. Of those that a mesh axis runs over, the one named last changes fastest.
Arguments:
- adjoint_now: float32 [4, 128, 64, 512], P('shot', 'space'), may hold values from -6 to 6
- adjoint_later: float32 [4, 128, 64, 512], P('shot', 'space'), may hold values from -6 to 6
- courant: float32 [128, 64, 512], P('space'), may hold values from 0.05 to 0.2
- checkpoint_codes: int32 [4, 6, 128, 64, 128], P('shot', None, 'space'), may hold values from -2147483648 to 2147483646
- scale_index: int32 [4, 6, 128, 256], P('shot', None, 'space'), may hold values from 0 to 63
- scale_table: float32 [64], replicated, may hold values from 0.001 to 0.01
- receiver_cell: int32 [4, 2048], P('shot', 'space'), may hold values from 0 to 4194303, as said below
- observed: float32 [4, 4, 2048], P('shot', None, 'space'), may hold values from -12 to 12
- source_cell: int32 [4, 3], P('shot'), may hold values from 0 to 511, as said below
Outputs:
- gradient: float32 [128, 64, 512], P('space', 'shot')
- adjoint_first: float32 [4, 128, 64, 512], P('shot', 'space')
- adjoint_second: float32 [4, 128, 64, 512], P('shot', 'space')
- misfit: float32 [], replicated
The draws below stay inside these ranges and needn't reach their ends.
Inputs may be any that keep to these rules, and one draw needn't show every extreme that they name: `receiver_cell`: for every r, entries r * 256 to (r + 1) * 256 - 1 of each shot's row are flat indices (z * 64 + y) * 512 + x of cells with r * 16 <= z < (r + 1) * 16. `source_cell`: column 0 is a z index below 128, column 1 a y index below 64, column 2 an x index below 512.
All inputs are finite; a program needn't handle non-finite values.
Results may differ from the reference program's by a relative error of at most 0.0001.
Values sent between devices are 32-bit elements; how exact they have to be, the bound alone decides.
A program may use at most 128 MiB of HBM per device.

```python
import math
import jax
import jax.numpy as jnp

NX = 512
NY = 64
CZ = 16
ITERS = 4
QBLOCK = 128
SCALES = 64
MUTE = 8
REC_DEV = 256
LEVELS = 6
NZ = 128
SHOTS = 4
RECEIVERS = 2048


def draw_receiver_cell(key, part):
    keys = jax.random.split(jax.random.fold_in(key, 11), 3)
    slab = jnp.arange(RECEIVERS, dtype=jnp.int32) // REC_DEV
    depth = slab * CZ + jax.random.randint(keys[0], (SHOTS, RECEIVERS), 0, CZ)
    row = jax.random.randint(keys[1], (SHOTS, RECEIVERS), 0, NY)
    col = jax.random.randint(keys[2], (SHOTS, RECEIVERS), 0, NX)
    return ((depth * NY + row) * NX + col).astype(jnp.int32)


def draw_observed(key, part):
    ramp = 1.0 + 2.0 * jnp.arange(RECEIVERS, dtype=jnp.float32) / RECEIVERS
    base = jnp.clip(jax.random.normal(jax.random.fold_in(key, 22), (SHOTS, ITERS, RECEIVERS), jnp.float32), -4.0, 4.0)
    return (base * ramp).astype(jnp.float32)


def draw_source_cell(key, part):
    keys = jax.random.split(jax.random.fold_in(key, 31), 4)
    depth = jax.random.randint(keys[0], (SHOTS, 1), 0, NZ)
    row = jax.random.randint(keys[1], (SHOTS, 1), 0, NY)
    col = jax.random.randint(keys[2], (SHOTS, 1), 0, NX)
    chosen = jax.random.randint(keys[3], (), 0, SHOTS)
    marked = (jnp.arange(SHOTS, dtype=jnp.int32) == chosen).reshape(SHOTS, 1)
    depth = jnp.where(marked, NZ - 1, depth)
    row = jnp.where(marked, 0, row)
    return jnp.concatenate([depth, row, col], axis=1).astype(jnp.int32)


def set_ends(entries, key, smallest, largest):
    index_at = [jax.random.randint(jax.random.fold_in(key, axis), (), 0, length) for axis, length in enumerate(entries.shape)]
    longest = entries.shape.index(max(entries.shape))
    neighbour = index_at[:longest] + [(index_at[longest] + 1) % entries.shape[longest]] + index_at[longest + 1:]
    return entries.at[tuple(index_at)].set(smallest).at[tuple(neighbour)].set(largest)


def block_scale(rng, dims, cuts, low, high):
    loudness = 1.0
    for dim, parts in cuts:
        draws = jax.random.uniform(jax.random.fold_in(jax.random.fold_in(rng, 6), dim), (parts,), jnp.float32, low / len(cuts), high / len(cuts))
        loudness = loudness * jnp.repeat(jnp.exp(draws), dims[dim] // parts).reshape((-1,) + (1,) * (len(dims) - 1 - dim))
    return loudness


def scatter_about(key, shape, width, limit, shards=(), kind=jnp.bfloat16):
    gain = block_scale(key, shape, shards, -0.22, 0.18) if shards else 1.0
    values = jax.random.normal(key, shape, jnp.float32) * width * gain
    return jnp.minimum(jnp.maximum(values, -limit), limit).astype(kind)


def setup_inputs(seed: int = 0) -> dict:
    seeds = jax.random.split(jax.random.key(seed), 10)
    return {
        "adjoint_now": scatter_about(seeds[0], (SHOTS, NZ, NY, NX), 1.0, 6.0, ((0, 4), (1, 8)), jnp.float32),
        "adjoint_later": scatter_about(seeds[1], (SHOTS, NZ, NY, NX), 1.0, 6.0, ((0, 4), (1, 8)), jnp.float32),
        "courant": jnp.clip(jnp.exp(math.log(0.2) - 1.3862944 * jax.random.uniform(seeds[2], (NZ, NY, NX), jnp.float32) ** block_scale(seeds[2], (NZ, NY, NX), ((0, 8),), -0.2, 0.2)), 0.05, 0.2),
        "checkpoint_codes": set_ends(jax.random.randint(seeds[3], (SHOTS, LEVELS, NZ, NY, NX // 4), -2147483648, 2147483647), jax.random.fold_in(seeds[3], 1), -2147483648, 2147483646).astype(jnp.int32),
        "scale_index": set_ends(jax.random.randint(seeds[4], (SHOTS, LEVELS, NZ, NY * NX // QBLOCK), 0, SCALES), jax.random.fold_in(seeds[4], 1), 0, SCALES - 1).astype(jnp.int32),
        "scale_table": jnp.clip(jnp.exp(jax.random.uniform(seeds[5], (SCALES,), jnp.float32, math.log(0.001), math.log(0.01))), 0.001, 0.01),
        "receiver_cell": draw_receiver_cell(jax.random.fold_in(seeds[9], 71), 0),
        "observed": draw_observed(jax.random.fold_in(seeds[9], 71), 0),
        "source_cell": draw_source_cell(jax.random.fold_in(seeds[9], 71), 0),
    }


COEFFS = (-205.0 / 72.0, 8.0 / 5.0, -1.0 / 5.0, 8.0 / 315.0, -1.0 / 560.0)


def decode(words, index, table):
    planes = [jnp.bitwise_and(jnp.right_shift(words, 8 * m), 255) for m in range(4)]
    codes = jnp.concatenate(planes, axis=-1)
    centred = (codes - 128).astype(jnp.float32)
    depth, rows, cols = centred.shape
    scale = table[index]
    blocks = centred.reshape(depth, rows, cols // QBLOCK, QBLOCK) * scale.reshape(depth, rows, cols // QBLOCK, 1)
    return blocks.reshape(depth, rows, cols)


def laplace(field):
    padded = jnp.pad(field, 4)
    depth, rows, cols = field.shape
    total = 3.0 * COEFFS[0] * field
    for step in range(1, 5):
        total = total + COEFFS[step] * (padded[4 + step:4 + step + depth, 4:4 + rows, 4:4 + cols] + padded[4 - step:4 - step + depth, 4:4 + rows, 4:4 + cols])
        total = total + COEFFS[step] * (padded[4:4 + depth, 4 + step:4 + step + rows, 4:4 + cols] + padded[4:4 + depth, 4 - step:4 - step + rows, 4:4 + cols])
        total = total + COEFFS[step] * (padded[4:4 + depth, 4:4 + rows, 4 + step:4 + step + cols] + padded[4:4 + depth, 4:4 + rows, 4 - step:4 - step + cols])
    return total


def reference(adjoint_now, adjoint_later, courant, checkpoint_codes, scale_index, scale_table, receiver_cell, observed, source_cell):
    gradient = jnp.zeros((NZ, NY, NX), jnp.float32)
    misfit_sum = jnp.zeros((), jnp.float32)
    firsts = []
    seconds = []
    zpos = jnp.arange(NZ, dtype=jnp.int32).reshape(NZ, 1, 1)
    ypos = jnp.arange(NY, dtype=jnp.int32).reshape(1, NY, 1)
    xpos = jnp.arange(NX, dtype=jnp.int32).reshape(1, 1, NX)
    for shot in range(SHOTS):
        fields = [decode(checkpoint_codes[shot, level], scale_index[shot, level], scale_table) for level in range(ITERS + 2)]
        now = adjoint_now[shot]
        later = adjoint_later[shot]
        image = jnp.zeros((NZ, NY, NX), jnp.float32)
        cells = receiver_cell[shot]
        for step in range(ITERS):
            level = ITERS - step
            synthetic = jnp.take(fields[level].reshape(-1), cells)
            residual = synthetic - observed[shot, level - 1]
            misfit_sum = misfit_sum + jnp.sum(residual * residual)
            image = image + now * (fields[level + 1] - 2.0 * fields[level] + fields[level - 1])
            stepped = 2.0 * now - later + courant * laplace(now)
            stepped = stepped.reshape(-1).at[cells].add(residual).reshape(NZ, NY, NX)
            later = now
            now = stepped
        source = source_cell[shot]
        dist = ((zpos - source[0]) ** 2 + (ypos - source[1]) ** 2 + (xpos - source[2]) ** 2).astype(jnp.float32)
        mute = 1.0 - jnp.exp(-dist / (2.0 * MUTE * MUTE))
        gradient = gradient + image * mute
        firsts.append(now)
        seconds.append(later)
    misfit = 0.5 * misfit_sum / (SHOTS * ITERS * RECEIVERS)
    return gradient, jnp.stack(firsts), jnp.stack(seconds), misfit
```

```python
import functools

import jax
import jax.numpy as jnp
from jax import lax
from jax.experimental import pallas as pl
from jax.experimental.pallas import tpu as pltpu
from jax.sharding import PartitionSpec as P

ITERS = 4
QBLOCK = 128
MUTE = 8
W = 4
NC = 2
F32 = jnp.float32
BF16 = jnp.bfloat16
MESH = pl.DeviceIdType.MESH

COEFFS = (-205.0 / 72.0, 8.0 / 5.0, -1.0 / 5.0, 8.0 / 315.0, -1.0 / 560.0)


def split(value):
    high = value.astype(BF16)
    return high, (value - high.astype(F32)).astype(BF16)


def dot(a, b):
    return jnp.dot(a, b, preferred_element_type=F32)


def band(rows, cols, first):
    i = first + lax.broadcasted_iota(jnp.int32, (rows, cols), 0)
    j = lax.broadcasted_iota(jnp.int32, (rows, cols), 1)
    d = jnp.abs(i - j)
    value = jnp.zeros((rows, cols), F32)
    for k in range(1, 5):
        value = jnp.where(d == k, COEFFS[k], value)
    return split(value)


def kernel(
    nshot,
    nspace,
    cells_s,
    source_s,
    table,
    observed,
    now_h,
    later_h,
    cour_h,
    words_h,
    index,
    cells_row,
    grad,
    first,
    second,
    misfit,
    E,
    D,
    cour,
    words,
    SC,
    TS,
    PC,
    OB,
    IM,
    RA,
    S,
    RB,
    PR,
    QH,
    QL,
    CH,
    CL,
    GW,
    GS,
    MB,
    SB,
    MT,
    ST,
    RL,
    halo_send,
    halo_recv,
    relay_recv,
    relay_send,
    a_send,
    a_recv,
    b_send,
    b_recv,
    m_send,
    m_recv,
    s_send,
    s_recv,
    local_sem,
):
    depth, rows, cols = cour.shape
    nrec = cells_row.shape[1]
    blocks = cols // QBLOCK
    ych = rows // NC
    shot = lax.axis_index("shot")
    space = lax.axis_index("space")
    has_low = space > 0
    has_high = space < nspace - 1

    barrier = pltpu.get_barrier_semaphore()
    for d in range(1, nshot):
        pl.semaphore_signal(
            barrier, inc=1, device_id={"shot": lax.rem(shot + d, nshot)}, device_id_type=MESH
        )

    @pl.loop(1, nspace)
    def _(d):
        pl.semaphore_signal(
            barrier, inc=1, device_id={"space": lax.rem(space + d, nspace)}, device_id_type=MESH
        )

    edge_low = pltpu.make_async_copy(
        now_h.at[pl.ds(0, W)], E.at[1, pl.ds(W, W)], local_sem.at[4]
    )
    edge_high = pltpu.make_async_copy(
        now_h.at[pl.ds(depth - W, W)], E.at[1, pl.ds(depth, W)], local_sem.at[5]
    )
    inner = depth - 2 * W
    in_now = pltpu.make_async_copy(
        now_h.at[pl.ds(W, inner)], E.at[1, pl.ds(2 * W, inner)], local_sem.at[0]
    )
    in_later = pltpu.make_async_copy(later_h, E.at[0, pl.ds(W, depth)], local_sem.at[1])
    in_cour = pltpu.make_async_copy(cour_h, cour, local_sem.at[2])
    in_words = pltpu.make_async_copy(words_h, words, local_sem.at[3])
    edge_low.start()
    edge_high.start()
    in_words.start()
    in_now.start()
    in_cour.start()
    in_later.start()

    edge_low.wait()
    edge_high.wait()
    pl.semaphore_wait(barrier, nshot + nspace - 2)

    odd = lax.rem(space, 2)
    column = space // 2
    columns = nspace // 2
    lean = W * (columns - 1 - column) // columns
    full = W * column // columns
    n_out = jnp.where(odd == 1, lean, full)
    n_in = jnp.where(odd == 1, full, lean)
    n_up = odd * n_out
    n_down = (1 - odd) * n_out
    most = RL.shape[2]

    def rows_of(c):
        return pl.ds(c * ych, ych)

    def halo(t, c, p, up):
        src_z = depth + p if up else W + p
        dst_z = p if up else W + depth + p
        return pltpu.make_async_remote_copy(
            src_ref=E.at[t + 1, src_z, rows_of(c), :],
            dst_ref=E.at[t + 1, dst_z, rows_of(c), :],
            send_sem=halo_send.at[int(up), t, c, p],
            recv_sem=halo_recv.at[int(up), t, c, p],
            device_id={"space": space + (1 if up else -1)},
            device_id_type=MESH,
        )

    def detour(t, c, p):
        return pltpu.make_async_remote_copy(
            src_ref=E.at[t + 1, W + p + odd * (depth - W), rows_of(c), :],
            dst_ref=RL.at[t, c, p],
            send_sem=halo_send.at[odd, t, c, p],
            recv_sem=relay_recv.at[t, c, p],
            device_id={"space": space + 1 - 2 * odd},
            device_id_type=MESH,
        )

    def onward(t, c, p):
        return pltpu.make_async_remote_copy(
            src_ref=RL.at[t, c, p],
            dst_ref=E.at[t + 1, p + odd * (W + depth), rows_of(c), :],
            send_sem=relay_send.at[t, c, p],
            recv_sem=halo_recv.at[1 - odd, t, c, p],
            device_id={"space": space + 2 - 4 * odd},
            device_id_type=MESH,
        )

    def send(t, c):
        for p in range(most):

            @pl.when(p < n_out)
            def _():
                detour(t, c, p).start()

        for p in range(W):

            @pl.when(jnp.logical_and(has_high, p >= n_up))
            def _():
                halo(t, c, p, True).start()

            @pl.when(jnp.logical_and(has_low, p >= n_down))
            def _():
                halo(t, c, p, False).start()

    def relay(t, c):
        for p in range(most):

            @pl.when(p < n_in)
            def _():
                detour(t, c, p).wait_recv()
                onward(t, c, p).start()

    for c in range(NC):
        send(0, c)

    @pl.loop(0, cols // 64)
    def _(i):
        start = pl.multiple_of(i * 64, 64)
        high, low = band(64, cols, start)
        CH[pl.ds(start, 64), :] = high
        CL[pl.ds(start, 64), :] = low

    yh, yl = band(rows, rows, 0)

    entry = index[...]
    scale = jnp.zeros(entry.shape, F32)
    for e in range(table.shape[0]):
        scale = jnp.where(entry == e, table[e], scale)
    levels = entry.shape[0]
    SC[0:levels] = scale
    SC[levels:] = jnp.zeros((SC.shape[0] - levels,) + entry.shape[1:], F32)

    slab = depth * rows * cols
    in_words.wait()

    @pl.loop(0, nrec, unroll=4)
    def _(r):
        cell = lax.rem(cells_s[r], slab)
        row = cell // cols
        z = row // rows
        y = lax.rem(row, rows)
        for k in range(1, ITERS + 1):
            GW[k - 1, pl.ds(r, 1), :] = words[k, z, pl.ds(y, 1), :]
            GS[k - 1, pl.ds(r, 1), :] = SC[k, pl.ds(z, 1), :]
            OB[k - 1, pl.ds(r, 1), :] = jnp.full((1, 128), observed[k - 1, r], F32)
        PC[pl.ds(r, 1), :] = jnp.full((1, 128), cell - z * (rows * cols), jnp.int32)

    place = PC[:, 0:1]
    xcol = lax.rem(place, cols)
    mcol = xcol // QBLOCK
    jcol = lax.rem(xcol, QBLOCK)
    scol = place // cols * blocks + mcol
    lane = lax.broadcasted_iota(jnp.int32, (nrec, QBLOCK), 1)
    sl = lax.broadcasted_iota(jnp.int32, (nrec, rows * blocks), 1)
    xl = lax.broadcasted_iota(jnp.int32, (nrec, cols), 1)
    squares = jnp.zeros((1, 1), F32)
    for k in range(1, ITERS + 1):
        code = jnp.bitwise_and(jnp.right_shift(GW[k - 1], 8 * mcol), 255) - 128
        code = jnp.sum(jnp.where(lane == jcol, code.astype(F32), 0.0), axis=1, keepdims=True)
        scale = jnp.sum(jnp.where(sl == scol, GS[k - 1], 0.0), axis=1, keepdims=True)
        residual = code * scale - OB[k - 1, :, 0:1]
        squares = squares + jnp.sum(residual * residual, axis=0, keepdims=True)
        high, low = split(jnp.where(xl == xcol, residual, 0.0))
        QH[ITERS - k] = high
        QL[ITERS - k] = low
    crow = lax.rem(cells_row[...], slab) // cols
    for z in range(depth):
        i = z * rows + lax.broadcasted_iota(jnp.int32, (rows, nrec), 0)
        PR[z] = jnp.where(i == crow, 1.0, 0.0).astype(BF16)

    tile = jnp.broadcast_to(squares, (8, 128))
    MT[...] = tile
    MB[pl.ds(shot, 1)] = tile.reshape(1, 8, 128)

    def misfit_copy(d):
        return pltpu.make_async_remote_copy(
            src_ref=MT,
            dst_ref=MB.at[shot],
            send_sem=m_send.at[d - 1],
            recv_sem=m_recv.at[d - 1],
            device_id={"shot": lax.rem(shot + d, nshot)},
            device_id_type=MESH,
        )

    def total_copy(d):
        return pltpu.make_async_remote_copy(
            src_ref=ST,
            dst_ref=SB.at[space],
            send_sem=s_send.at[d - 1],
            recv_sem=s_recv.at[d - 1],
            device_id={"space": lax.rem(space + d, nspace)},
            device_id_type=MESH,
        )

    for d in range(1, nshot):
        misfit_copy(d).start()

    relay(0, 0)
    in_now.wait()
    in_later.wait()
    in_cour.wait()

    def local(t):
        for g in (0, depth // W - 1) + tuple(range(1, depth // W - 1)):
            z0 = g * W
            u = E[t + 1, W + z0 : W + z0 + W].reshape(W * rows, cols)
            uh, ul = split(u)
            lap = dot(uh, CH[...]) + dot(ul, CH[...]) + dot(uh, CL[...])
            for j in range(W):
                z = z0 + j
                part = slice(j * rows, (j + 1) * rows)
                up = u[part]
                acc = lap[part] + (3.0 * COEFFS[0]) * up
                acc = acc + dot(yh, uh[part]) + dot(yh, ul[part]) + dot(yl, uh[part])
                for i in range(1, 5):
                    if z + i < depth:
                        acc = acc + COEFFS[i] * E[t + 1, W + z + i]
                    if z - i >= 0:
                        acc = acc + COEFFS[i] * E[t + 1, W + z - i]
                inject = dot(PR[z], QH[t]) + dot(PR[z], QL[t])
                E[t + 2, W + z] = 2.0 * up - E[t, W + z] + cour[z] * acc + inject

    def spread():
        i = lax.broadcasted_iota(jnp.int32, (rows, rows * blocks), 0)
        j = lax.broadcasted_iota(jnp.int32, (rows, rows * blocks), 1)
        flat = SC[...].reshape(128, rows * blocks)
        high = flat.astype(BF16)
        rest = flat - high.astype(F32)
        pieces = (high,) + split(rest)
        for m in range(blocks):
            pick = jnp.where(j == blocks * i + m, 1.0, 0.0).astype(BF16)
            moved = jnp.zeros((rows, 128), F32)
            for piece in pieces:
                moved = moved + lax.dot_general(
                    pick, piece, (((1,), (1,)), ((), ())), preferred_element_type=F32
                )
            TS[m] = moved

    def decode(part):
        @pl.loop(0, depth // 4)
        def _(step):
            z = part * (depth // 4) + step
            for m in range(blocks):
                xs = slice(m * QBLOCK, (m + 1) * QBLOCK)
                scale = pltpu.roll(TS[m], lax.rem(128 - z, 128), 1)
                f = []
                for k in range(ITERS + 2):
                    code = jnp.bitwise_and(jnp.right_shift(words[k, z], 8 * m), 255) - 128
                    f.append(code.astype(F32) * scale[:, k * depth : k * depth + 1])
                for t in range(ITERS):
                    k = ITERS - t
                    diff = f[k + 1] - 2.0 * f[k] + f[k - 1]
                    if t == 0:
                        IM[z, :, xs] = E[1, W + z, :, xs] * diff
                    else:
                        D[t - 1, z, :, xs] = diff

    spread()
    local(0)

    for d in range(1, nshot):
        misfit_copy(d).wait()
    total = MB[0]
    for d in range(1, nshot):
        total = total + MB[d]
    ST[...] = total
    SB[pl.ds(space, 1)] = total.reshape(1, 8, 128)

    @pl.loop(1, nspace)
    def _(d):
        total_copy(d).start()

    def fix(t, c, target, base):
        ys = rows_of(c)

        @pl.when(has_low)
        def _():
            for p in range(W):
                halo(t, c, p, True).wait_recv()
            for j in range(W):
                acc = COEFFS[j + 1] * E[t + 1, W - 1, ys, :]
                for i in range(j + 2, 5):
                    acc = acc + COEFFS[i] * E[t + 1, W + j - i, ys, :]
                target[base + j, ys, :] += cour[j, ys, :] * acc

        @pl.when(has_high)
        def _():
            for p in range(W):
                halo(t, c, p, False).wait_recv()
            for j in range(W):
                z = depth - 1 - j
                acc = COEFFS[j + 1] * E[t + 1, W + depth, ys, :]
                for i in range(j + 2, 5):
                    acc = acc + COEFFS[i] * E[t + 1, W + z + i, ys, :]
                target[base + z, ys, :] += cour[z, ys, :] * acc

    first_z = space * depth
    core = lax.rem(shot, 2)
    pair = shot // 2
    pairs = nshot // 2
    yq = rows // nshot
    pieces = ((W, inner), (0, W), (depth - W, W))

    def quarter(index):
        return pl.ds(pl.multiple_of(index * yq, yq), yq)

    def mute(z):
        dz = first_z + z - source_s[0]
        dy = lax.broadcasted_iota(jnp.int32, (rows, cols), 0) - source_s[1]
        dx = lax.broadcasted_iota(jnp.int32, (rows, cols), 1) - source_s[2]
        dist = (dz * dz + dy * dy + dx * dx).astype(F32)
        IM[z] = IM[z] * (1.0 - jnp.exp(dist * (-1.0 / (2.0 * MUTE * MUTE))))

    def copy_a(h, n):
        at = pl.ds(*pieces[n])
        return pltpu.make_async_remote_copy(
            src_ref=IM.at[at, quarter(2 * h + 1 - core), :],
            dst_ref=RA.at[h, at],
            send_sem=a_send.at[h, n],
            recv_sem=a_recv.at[h, n],
            device_id={"shot": shot + 1 - 2 * core},
            device_id_type=MESH,
        )

    def copy_b(d, n):
        at = pl.ds(*pieces[n])
        other = lax.rem(pair + d, pairs)
        return pltpu.make_async_remote_copy(
            src_ref=S.at[other, at],
            dst_ref=RB.at[d - 1, at],
            send_sem=b_send.at[d - 1, n],
            recv_sem=b_recv.at[d - 1, n],
            device_id={"shot": 2 * other + core},
            device_id_type=MESH,
        )

    def offer(n):
        for h in range(pairs):
            copy_a(h, n).start()

    def pass_on(n):
        at = pl.ds(*pieces[n])
        for h in range(pairs):
            copy_a(h, n).wait()
            S[h, at] = IM[at, quarter(2 * h + core), :] + RA[h, at]
        for d in range(1, pairs):
            copy_b(d, n).start()

    @pl.loop(0, ITERS - 1)
    def _(t):
        fix(t, 0, E.at[t + 2], W)
        send(t + 1, 0)

        @pl.when(t < 2)
        def _():
            decode(2 * t)

        relay(t, 1)

        @pl.when(t < 2)
        def _():
            decode(2 * t + 1)

        @pl.when(t == ITERS - 2)
        def _():
            pass_on(0)

        fix(t, 1, E.at[t + 2], W)
        send(t + 1, 1)

        @pl.when(t == ITERS - 2)
        def _():
            for low in (0, depth - W):

                @pl.loop(low, low + W)
                def _(z):
                    IM[z] = IM[z] + E[ITERS, W + z] * D[ITERS - 2, z]
                    mute(z)

            offer(1)
            offer(2)

        local(t + 1)
        relay(t + 1, 0)

        @pl.when(t == ITERS - 3)
        def _():
            @pl.loop(0, depth)
            def _(z):
                value = IM[z]
                for k in range(ITERS - 2):
                    value = value + E[k + 2, W + z] * D[k, z]
                IM[z] = value

            @pl.loop(W, depth - W)
            def _(z):
                IM[z] = IM[z] + E[ITERS, W + z] * D[ITERS - 2, z]
                mute(z)

            offer(0)

    pass_on(1)
    pass_on(2)

    @pl.loop(0, depth)
    def _(z):
        second[z] = E[ITERS, W + z]
        first[z] = E[ITERS + 1, W + z]

    fix(ITERS - 1, 0, first, 0)
    relay(ITERS - 1, 1)
    fix(ITERS - 1, 1, first, 0)

    total = S[pair]
    for d in range(1, pairs):
        for n in range(len(pieces)):
            copy_b(d, n).wait()
        total = total + RB[d - 1]
    grad[...] = total

    @pl.loop(1, nspace)
    def _(d):
        total_copy(d).wait()

    whole = SB[0]
    for d in range(1, nspace):
        whole = whole + SB[d]
    misfit[...] = whole

    @pl.loop(0, ITERS)
    def _(t):
        for c in range(NC):
            for p in range(W):

                @pl.when(has_high)
                def _():
                    halo(t, c, p, True).wait_send()

                @pl.when(has_low)
                def _():
                    halo(t, c, p, False).wait_send()

            for p in range(most):

                @pl.when(p < n_in)
                def _():
                    onward(t, c, p).wait_send()


def finish(factor, grad, first, second, total, grad_o, first_o, second_o, misfit, sem):
    copies = [
        pltpu.make_async_copy(source, target, sem.at[n])
        for n, (source, target) in enumerate(((first, first_o), (second, second_o), (grad, grad_o)))
    ]
    for copy in copies:
        copy.start()
    misfit[...] = total[0:1, 0:1] * factor
    for copy in copies:
        copy.wait()


def body(
    nshot,
    nspace,
    adjoint_now,
    adjoint_later,
    courant,
    checkpoint_codes,
    scale_index,
    scale_table,
    receiver_cell,
    observed,
    source_cell,
):
    depth, rows, cols = courant.shape
    levels = checkpoint_codes.shape[1]
    nrec = receiver_cell.shape[1]
    blocks = cols // QBLOCK
    pairs = nshot // 2
    yq = rows // nshot
    vmem = pl.BlockSpec(memory_space=pltpu.VMEM)
    smem = pl.BlockSpec(memory_space=pltpu.SMEM)
    anyspace = pl.BlockSpec(memory_space=pltpu.HBM)
    dma = pltpu.SemaphoreType.DMA
    held = pltpu.VMEM((depth, rows, cols), F32)
    field = jax.ShapeDtypeStruct((depth, rows, cols), F32)
    columns = nspace // 2
    most = max(W * (columns - 1) // columns, 1)
    gradient, first, second, total = pl.pallas_call(
        functools.partial(kernel, nshot, nspace),
        out_shape=(
            pltpu.VMEM((depth, yq, cols), F32),
            held,
            held,
            pltpu.VMEM((8, 128), F32),
        ),
        in_specs=[smem] * 4 + [anyspace] * 4 + [vmem] * 2,
        out_specs=(vmem, vmem, vmem, vmem),
        scratch_shapes=[
            pltpu.VMEM((ITERS + 2, depth + 2 * W, rows, cols), F32),
            pltpu.VMEM((ITERS - 1, depth, rows, cols), F32),
            pltpu.VMEM((depth, rows, cols), F32),
            pltpu.VMEM((levels, depth, rows, QBLOCK), jnp.int32),
            pltpu.VMEM((128 // depth, depth, rows * blocks), F32),
            pltpu.VMEM((blocks, rows, 128), F32),
            pltpu.VMEM((nrec, 128), jnp.int32),
            pltpu.VMEM((ITERS, nrec, 128), F32),
            pltpu.VMEM((depth, rows, cols), F32),
            pltpu.VMEM((pairs, depth, yq, cols), F32),
            pltpu.VMEM((pairs, depth, yq, cols), F32),
            pltpu.VMEM((max(pairs - 1, 1), depth, yq, cols), F32),
            pltpu.VMEM((depth, rows, nrec), BF16),
            pltpu.VMEM((ITERS, nrec, cols), BF16),
            pltpu.VMEM((ITERS, nrec, cols), BF16),
            pltpu.VMEM((cols, cols), BF16),
            pltpu.VMEM((cols, cols), BF16),
            pltpu.VMEM((ITERS, nrec, QBLOCK), jnp.int32),
            pltpu.VMEM((ITERS, nrec, rows * blocks), F32),
            pltpu.VMEM((nshot, 8, 128), F32),
            pltpu.VMEM((nspace, 8, 128), F32),
            pltpu.VMEM((8, 128), F32),
            pltpu.VMEM((8, 128), F32),
            pltpu.VMEM((ITERS, NC, most, rows // NC, cols), F32),
            dma((2, ITERS, NC, W)),
            dma((2, ITERS, NC, W)),
            dma((ITERS, NC, most)),
            dma((ITERS, NC, most)),
            dma((pairs, 3)),
            dma((pairs, 3)),
            dma((max(pairs - 1, 1), 3)),
            dma((max(pairs - 1, 1), 3)),
            dma((nshot - 1,)),
            dma((nshot - 1,)),
            dma((nspace - 1,)),
            dma((nspace - 1,)),
            dma((6,)),
        ],
        compiler_params=pltpu.CompilerParams(
            collective_id=0, has_side_effects=True, vmem_limit_bytes=52000000
        ),
    )(
        receiver_cell[0],
        source_cell[0],
        scale_table,
        observed[0],
        adjoint_now[0],
        adjoint_later[0],
        courant,
        checkpoint_codes[0],
        scale_index[0],
        receiver_cell,
    )
    count = nshot * ITERS * nrec * nspace
    gradient, first, second, misfit = pl.pallas_call(
        functools.partial(finish, 0.5 / count),
        out_shape=(jax.ShapeDtypeStruct(gradient.shape, F32), field, field, jax.ShapeDtypeStruct((1, 1), F32)),
        in_specs=[vmem] * 4,
        out_specs=(anyspace, anyspace, anyspace, vmem),
        scratch_shapes=[dma((3,))],
        compiler_params=pltpu.CompilerParams(vmem_limit_bytes=16000000),
    )(gradient, first, second, total)
    return (gradient, first[None], second[None], misfit.reshape(()))


def solution(mesh):
    placed = (
        P("shot", "space", None, None),
        P("shot", "space", None, None),
        P("space", None, None),
        P("shot", None, "space", None, None),
        P("shot", None, "space", None),
        P(),
        P("shot", "space"),
        P("shot", None, "space"),
        P("shot", None),
    )
    return jax.shard_map(
        functools.partial(body, mesh.shape["shot"], mesh.shape["space"]),
        mesh=mesh,
        in_specs=placed,
        out_specs=(
            P("space", "shot", None),
            P("shot", "space", None, None),
            P("shot", "space", None, None),
            P(),
        ),
        check_vma=False,
    )
```

```python
import functools

import jax
import jax.numpy as jnp
from jax import lax
from jax.experimental import pallas as pl
from jax.experimental.pallas import tpu as pltpu
from jax.sharding import PartitionSpec as P

ITERS = 4
QBLOCK = 128
MUTE = 8
W = 4
NC = 2
F32 = jnp.float32
BF16 = jnp.bfloat16
MESH = pl.DeviceIdType.MESH

COEFFS = (-205.0 / 72.0, 8.0 / 5.0, -1.0 / 5.0, 8.0 / 315.0, -1.0 / 560.0)


def split(value):
    high = value.astype(BF16)
    return high, (value - high.astype(F32)).astype(BF16)


def dot(a, b):
    return jnp.dot(a, b, preferred_element_type=F32)


def band(rows, cols, first):
    i = first + lax.broadcasted_iota(jnp.int32, (rows, cols), 0)
    j = lax.broadcasted_iota(jnp.int32, (rows, cols), 1)
    d = jnp.abs(i - j)
    value = jnp.zeros((rows, cols), F32)
    for k in range(1, 5):
        value = jnp.where(d == k, COEFFS[k], value)
    return split(value)


def kernel(
    nshot,
    nspace,
    cells_h,
    source_h,
    table_h,
    observed_h,
    now_h,
    later_h,
    cour_h,
    words_h,
    index_h,
    grad,
    first,
    second,
    misfit,
    cells_s,
    source_s,
    table,
    observed,
    index,
    cells_row,
    E,
    D,
    cour,
    words,
    SC,
    TS,
    PC,
    OB,
    IM,
    RA,
    S,
    RB,
    PR,
    QH,
    QL,
    CH,
    CL,
    GW,
    GS,
    MB,
    MT,
    ST,
    PX,
    CO,
    CI,
    RL,
    halo_send,
    halo_recv,
    relay_recv,
    relay_send,
    a_send,
    a_recv,
    b_send,
    b_recv,
    m_send,
    m_recv,
    p_sem,
    s_send,
    s_recv,
    small_sem,
    local_sem,
):
    depth, rows, cols = cour.shape
    nrec = cells_row.shape[1]
    blocks = cols // QBLOCK
    ych = rows // NC
    shot = lax.axis_index("shot")
    space = lax.axis_index("space")
    has_low = space > 0
    has_high = space < nspace - 1

    barrier = pltpu.get_barrier_semaphore()
    for d in range(1, nshot):
        pl.semaphore_signal(
            barrier, inc=1, device_id={"shot": lax.rem(shot + d, nshot)}, device_id_type=MESH
        )

    near = ((-2, space >= 2), (-1, has_low), (1, has_high), (2, space < nspace - 2))
    for d, there in near:

        @pl.when(there)
        def _():
            pl.semaphore_signal(
                barrier, inc=1, device_id={"space": space + d}, device_id_type=MESH
            )

    edge_low = pltpu.make_async_copy(
        now_h.at[pl.ds(0, W)], E.at[1, pl.ds(W, W)], local_sem.at[4]
    )
    edge_high = pltpu.make_async_copy(
        now_h.at[pl.ds(depth - W, W)], E.at[1, pl.ds(depth, W)], local_sem.at[5]
    )
    inner = depth - 2 * W
    in_now = pltpu.make_async_copy(
        now_h.at[pl.ds(W, inner)], E.at[1, pl.ds(2 * W, inner)], local_sem.at[0]
    )
    in_later = pltpu.make_async_copy(later_h, E.at[0, pl.ds(W, depth)], local_sem.at[1])
    in_cour = pltpu.make_async_copy(cour_h, cour, local_sem.at[2])
    in_words = pltpu.make_async_copy(words_h, words, local_sem.at[3])
    edge_low.start()
    edge_high.start()
    in_words.start()
    in_now.start()
    in_cour.start()
    in_later.start()
    small = [
        pltpu.make_async_copy(source, target, small_sem.at[n])
        for n, (source, target) in enumerate(
            (
                (index_h, index),
                (cells_h, cells_row),
                (cells_h, cells_s),
                (source_h, source_s),
                (table_h, table),
                (observed_h, observed),
            )
        )
    ]
    for copy in small:
        copy.start()

    edge_low.wait()
    edge_high.wait()
    present = sum(there.astype(jnp.int32) for _, there in near)
    pl.semaphore_wait(barrier, nshot - 1 + present)

    odd = lax.rem(space, 2)
    column = space // 2
    columns = nspace // 2
    lean = W * (columns - 1 - column) // columns
    full = W * column // columns
    n_out = jnp.where(odd == 1, lean, full)
    n_in = jnp.where(odd == 1, full, lean)
    n_up = odd * n_out
    n_down = (1 - odd) * n_out
    most = RL.shape[2]

    def rows_of(c):
        return pl.ds(c * ych, ych)

    def halo(t, c, p, up, planes=1):
        src_z = depth + p if up else W + p
        dst_z = p if up else W + depth + p
        return pltpu.make_async_remote_copy(
            src_ref=E.at[t + 1, pl.ds(src_z, planes), rows_of(c), :],
            dst_ref=E.at[t + 1, pl.ds(dst_z, planes), rows_of(c), :],
            send_sem=halo_send.at[int(up), t, c],
            recv_sem=halo_recv.at[int(up), t, c],
            device_id={"space": space + (1 if up else -1)},
            device_id_type=MESH,
        )

    def detour(t, c, p):
        return pltpu.make_async_remote_copy(
            src_ref=E.at[t + 1, W + p + odd * (depth - W), rows_of(c), :],
            dst_ref=RL.at[t, c, p],
            send_sem=halo_send.at[odd, t, c],
            recv_sem=relay_recv.at[t, c, p],
            device_id={"space": space + 1 - 2 * odd},
            device_id_type=MESH,
        )

    def onward(t, c, p):
        return pltpu.make_async_remote_copy(
            src_ref=RL.at[t, c, p],
            dst_ref=E.at[t + 1, p + odd * (W + depth), rows_of(c), :],
            send_sem=relay_send.at[t, c, p],
            recv_sem=halo_recv.at[1 - odd, t, c],
            device_id={"space": space + 2 - 4 * odd},
            device_id_type=MESH,
        )

    def send(t, c):
        for p in range(most):

            @pl.when(p < n_out)
            def _():
                detour(t, c, p).start()

        for p in range(W):

            @pl.when(jnp.logical_and(has_high, p >= n_up))
            def _():
                halo(t, c, p, True).start()

            @pl.when(jnp.logical_and(has_low, p >= n_down))
            def _():
                halo(t, c, p, False).start()

    def relay(t, c):
        for p in range(most):

            @pl.when(p < n_in)
            def _():
                detour(t, c, p).wait_recv()
                onward(t, c, p).start()

    def drain(t, c):
        @pl.when(has_high)
        def _():
            halo(t, c, 0, True, W).wait_send()

        @pl.when(has_low)
        def _():
            halo(t, c, 0, False, W).wait_send()

        for p in range(most):

            @pl.when(p < n_in)
            def _():
                onward(t, c, p).wait_send()

    for c in range(NC):
        send(0, c)

    @pl.loop(0, cols // 64)
    def _(i):
        start = pl.multiple_of(i * 64, 64)
        high, low = band(64, cols, start)
        CH[pl.ds(start, 64), :] = high
        CL[pl.ds(start, 64), :] = low

    yh, yl = band(rows, rows, 0)
    for copy in small:
        copy.wait()

    entry = index[...]
    scale = jnp.zeros(entry.shape, F32)
    for e in range(table.shape[0]):
        scale = jnp.where(entry == e, table[e], scale)
    levels = entry.shape[0]
    SC[0:levels] = scale
    SC[levels:] = jnp.zeros((SC.shape[0] - levels,) + entry.shape[1:], F32)

    slab = depth * rows * cols
    in_words.wait()

    @pl.loop(0, nrec, unroll=4)
    def _(r):
        cell = lax.rem(cells_s[0, r], slab)
        row = cell // cols
        z = row // rows
        y = lax.rem(row, rows)
        for k in range(1, ITERS + 1):
            GW[k - 1, pl.ds(r, 1), :] = words[k, z, pl.ds(y, 1), :]
            GS[k - 1, pl.ds(r, 1), :] = SC[k, pl.ds(z, 1), :]
            OB[k - 1, pl.ds(r, 1), :] = jnp.full((1, 128), observed[k - 1, r], F32)
        PC[pl.ds(r, 1), :] = jnp.full((1, 128), cell - z * (rows * cols), jnp.int32)

    place = PC[:, 0:1]
    xcol = lax.rem(place, cols)
    mcol = xcol // QBLOCK
    jcol = lax.rem(xcol, QBLOCK)
    scol = place // cols * blocks + mcol
    lane = lax.broadcasted_iota(jnp.int32, (nrec, QBLOCK), 1)
    sl = lax.broadcasted_iota(jnp.int32, (nrec, rows * blocks), 1)
    xl = lax.broadcasted_iota(jnp.int32, (nrec, cols), 1)
    squares = jnp.zeros((1, 1), F32)
    for k in range(1, ITERS + 1):
        code = jnp.bitwise_and(jnp.right_shift(GW[k - 1], 8 * mcol), 255) - 128
        code = jnp.sum(jnp.where(lane == jcol, code.astype(F32), 0.0), axis=1, keepdims=True)
        scale = jnp.sum(jnp.where(sl == scol, GS[k - 1], 0.0), axis=1, keepdims=True)
        residual = code * scale - OB[k - 1, :, 0:1]
        squares = squares + jnp.sum(residual * residual, axis=0, keepdims=True)
        high, low = split(jnp.where(xl == xcol, residual, 0.0))
        QH[ITERS - k] = high
        QL[ITERS - k] = low
    crow = lax.rem(cells_row[...], slab) // cols
    for z in range(depth):
        i = z * rows + lax.broadcasted_iota(jnp.int32, (rows, nrec), 0)
        PR[z] = jnp.where(i == crow, 1.0, 0.0).astype(BF16)

    tile = jnp.broadcast_to(squares, (8, 128))
    MT[...] = tile
    MB[pl.ds(shot, 1)] = tile.reshape(1, 8, 128)

    def misfit_copy(d):
        return pltpu.make_async_remote_copy(
            src_ref=MT,
            dst_ref=MB.at[shot],
            send_sem=m_send.at[d - 1],
            recv_sem=m_recv.at[d - 1],
            device_id={"shot": lax.rem(shot + d, nshot)},
            device_id_type=MESH,
        )

    def pair_copy():
        return pltpu.make_async_remote_copy(
            src_ref=ST,
            dst_ref=PX,
            send_sem=p_sem.at[0],
            recv_sem=p_sem.at[1],
            device_id={"space": space + 1 - 2 * odd},
            device_id_type=MESH,
        )

    def chain_copy(way):
        return pltpu.make_async_remote_copy(
            src_ref=CO.at[way],
            dst_ref=CI.at[way],
            send_sem=s_send.at[way],
            recv_sem=s_recv.at[way],
            device_id={"space": space + (2 if way else -2)},
            device_id_type=MESH,
        )

    def chain(slot):
        for way in (0, 1):
            place = column if way else columns - 1 - column
            turn = jnp.logical_or(place == slot, jnp.logical_and(slot == 3, place > slot))

            @pl.when(turn)
            def _():
                @pl.when(place > 0)
                def _():
                    chain_copy(way).wait_recv()
                    CO[way] = CI[way]

                CO[way, pl.ds(column, 1)] = (ST[...] + PX[...]).reshape(1, 8, 128)

                @pl.when(place < columns - 1)
                def _():
                    chain_copy(way).start()

    for d in range(1, nshot):
        misfit_copy(d).start()

    relay(0, 0)
    in_now.wait()
    in_later.wait()
    in_cour.wait()

    groups = (0, depth // W - 1) + tuple(range(1, depth // W - 1))

    def local(t, chosen):
        for g in chosen:
            z0 = g * W
            u = E[t + 1, W + z0 : W + z0 + W].reshape(W * rows, cols)
            uh, ul = split(u)
            lap = dot(uh, CH[...]) + dot(ul, CH[...]) + dot(uh, CL[...])
            for j in range(W):
                z = z0 + j
                part = slice(j * rows, (j + 1) * rows)
                up = u[part]
                acc = lap[part] + (3.0 * COEFFS[0]) * up
                acc = acc + dot(yh, uh[part]) + dot(yh, ul[part]) + dot(yl, uh[part])
                for i in range(1, 5):
                    if z + i < depth:
                        acc = acc + COEFFS[i] * E[t + 1, W + z + i]
                    if z - i >= 0:
                        acc = acc + COEFFS[i] * E[t + 1, W + z - i]
                inject = dot(PR[z], QH[t]) + dot(PR[z], QL[t])
                E[t + 2, W + z] = 2.0 * up - E[t, W + z] + cour[z] * acc + inject

    def spread():
        i = lax.broadcasted_iota(jnp.int32, (rows, rows * blocks), 0)
        j = lax.broadcasted_iota(jnp.int32, (rows, rows * blocks), 1)
        flat = SC[...].reshape(128, rows * blocks)
        high = flat.astype(BF16)
        rest = flat - high.astype(F32)
        pieces = (high,) + split(rest)
        for m in range(blocks):
            pick = jnp.where(j == blocks * i + m, 1.0, 0.0).astype(BF16)
            moved = jnp.zeros((rows, 128), F32)
            for piece in pieces:
                moved = moved + lax.dot_general(
                    pick, piece, (((1,), (1,)), ((), ())), preferred_element_type=F32
                )
            TS[m] = moved

    def decode(part):
        @pl.loop(0, depth // 4)
        def _(step):
            z = part * (depth // 4) + step
            for m in range(blocks):
                xs = slice(m * QBLOCK, (m + 1) * QBLOCK)
                scale = pltpu.roll(TS[m], lax.rem(128 - z, 128), 1)
                f = []
                for k in range(ITERS + 2):
                    code = jnp.bitwise_and(jnp.right_shift(words[k, z], 8 * m), 255) - 128
                    f.append(code.astype(F32) * scale[:, k * depth : k * depth + 1])
                for t in range(ITERS):
                    k = ITERS - t
                    diff = f[k + 1] - 2.0 * f[k] + f[k - 1]
                    if t == 0:
                        IM[z, :, xs] = E[1, W + z, :, xs] * diff
                    else:
                        D[t - 1, z, :, xs] = diff

    spread()
    local(0, groups)

    for d in range(1, nshot):
        misfit_copy(d).wait()
    total = MB[0]
    for d in range(1, nshot):
        total = total + MB[d]
    ST[...] = total
    pair_copy().start()
    CO[...] = jnp.zeros(CO.shape, F32)

    def fix(t, c, target, base):
        ys = rows_of(c)

        @pl.when(has_low)
        def _():
            halo(t, c, 0, True, W).wait_recv()
            for j in range(W):
                acc = COEFFS[j + 1] * E[t + 1, W - 1, ys, :]
                for i in range(j + 2, 5):
                    acc = acc + COEFFS[i] * E[t + 1, W + j - i, ys, :]
                target[base + j, ys, :] += cour[j, ys, :] * acc

        @pl.when(has_high)
        def _():
            halo(t, c, 0, False, W).wait_recv()
            for j in range(W):
                z = depth - 1 - j
                acc = COEFFS[j + 1] * E[t + 1, W + depth, ys, :]
                for i in range(j + 2, 5):
                    acc = acc + COEFFS[i] * E[t + 1, W + z + i, ys, :]
                target[base + z, ys, :] += cour[z, ys, :] * acc

    first_z = space * depth
    core = lax.rem(shot, 2)
    pair = shot // 2
    pairs = nshot // 2
    yq = rows // nshot
    pieces = ((W, inner), (0, W), (depth - W, W))

    def quarter(index):
        return pl.ds(pl.multiple_of(index * yq, yq), yq)

    def mute(z):
        dz = first_z + z - source_s[0, 0]
        dy = lax.broadcasted_iota(jnp.int32, (rows, cols), 0) - source_s[0, 1]
        dx = lax.broadcasted_iota(jnp.int32, (rows, cols), 1) - source_s[0, 2]
        dist = (dz * dz + dy * dy + dx * dx).astype(F32)
        IM[z] = IM[z] * (1.0 - jnp.exp(dist * (-1.0 / (2.0 * MUTE * MUTE))))

    def copy_a(h, n):
        at = pl.ds(*pieces[n])
        return pltpu.make_async_remote_copy(
            src_ref=IM.at[at, quarter(2 * h + 1 - core), :],
            dst_ref=RA.at[h, at],
            send_sem=a_send.at[h, n],
            recv_sem=a_recv.at[h, n],
            device_id={"shot": shot + 1 - 2 * core},
            device_id_type=MESH,
        )

    def copy_b(d, n):
        at = pl.ds(*pieces[n])
        other = lax.rem(pair + d, pairs)
        return pltpu.make_async_remote_copy(
            src_ref=S.at[other, at],
            dst_ref=RB.at[d - 1, at],
            send_sem=b_send.at[d - 1, n],
            recv_sem=b_recv.at[d - 1, n],
            device_id={"shot": 2 * other + core},
            device_id_type=MESH,
        )

    def offer(n):
        for h in range(pairs):
            copy_a(h, n).start()

    def pass_on(n):
        at = pl.ds(*pieces[n])
        for h in range(pairs):
            copy_a(h, n).wait()
            S[h, at] = IM[at, quarter(2 * h + core), :] + RA[h, at]
        for d in range(1, pairs):
            copy_b(d, n).start()

    @pl.loop(0, ITERS - 1)
    def _(t):
        fix(t, 0, E.at[t + 2], W)
        send(t + 1, 0)

        @pl.when(t == 1)
        def _():
            pair_copy().wait()

        @pl.when(t > 0)
        def _():
            chain(2 * t - 2)

        @pl.when(t < 2)
        def _():
            decode(2 * t)

        relay(t, 1)

        @pl.when(t < 2)
        def _():
            decode(2 * t + 1)

        @pl.when(t == ITERS - 2)
        def _():
            pass_on(0)

        fix(t, 1, E.at[t + 2], W)
        send(t + 1, 1)

        @pl.when(t == ITERS - 2)
        def _():
            for low in (0, depth - W):

                @pl.loop(low, low + W)
                def _(z):
                    IM[z] = IM[z] + E[ITERS, W + z] * D[ITERS - 2, z]
                    mute(z)

            offer(1)
            offer(2)

        local(t + 1, groups[:2])
        relay(t + 1, 0)

        @pl.when(t == ITERS - 2)
        def _():
            pass_on(1)
            pass_on(2)

        local(t + 1, groups[2:])

        @pl.when(t > 0)
        def _():
            chain(2 * t - 1)

        drain(t, 0)
        drain(t, 1)

        @pl.when(t == ITERS - 3)
        def _():
            @pl.loop(0, depth)
            def _(z):
                value = IM[z]
                for k in range(ITERS - 2):
                    value = value + E[k + 2, W + z] * D[k, z]
                IM[z] = value

            @pl.loop(W, depth - W)
            def _(z):
                IM[z] = IM[z] + E[ITERS, W + z] * D[ITERS - 2, z]
                mute(z)

            offer(0)

    @pl.loop(0, depth)
    def _(z):
        second[z] = E[ITERS, W + z]
        first[z] = E[ITERS + 1, W + z]

    fix(ITERS - 1, 0, first, 0)
    relay(ITERS - 1, 1)
    drain(ITERS - 1, 0)
    fix(ITERS - 1, 1, first, 0)

    total = S[pair]
    for d in range(1, pairs):
        for n in range(len(pieces)):
            copy_b(d, n).wait()
        total = total + RB[d - 1]
    grad[...] = total

    whole = jnp.zeros((8, 128), F32)
    for way in (0, 1):
        @pl.when(column != (columns - 1 if way else 0))
        def _():
            chain_copy(way).wait_send()

    @pl.when(column < columns - 1)
    def _():
        CO[1] = CO[1] + CI[0]

    for k in range(columns):
        whole = whole + CO[1, k]
    misfit[...] = whole

    drain(ITERS - 1, 1)


def finish(factor, grad, first, second, total, grad_o, first_o, second_o, misfit, sem):
    copies = [
        pltpu.make_async_copy(source, target, sem.at[n])
        for n, (source, target) in enumerate(((first, first_o), (second, second_o), (grad, grad_o)))
    ]
    for copy in copies:
        copy.start()
    misfit[...] = total[0:1, 0:1] * factor
    for copy in copies:
        copy.wait()


def body(
    nshot,
    nspace,
    adjoint_now,
    adjoint_later,
    courant,
    checkpoint_codes,
    scale_index,
    scale_table,
    receiver_cell,
    observed,
    source_cell,
):
    depth, rows, cols = courant.shape
    levels = checkpoint_codes.shape[1]
    nrec = receiver_cell.shape[1]
    blocks = cols // QBLOCK
    pairs = nshot // 2
    yq = rows // nshot
    vmem = pl.BlockSpec(memory_space=pltpu.VMEM)
    anyspace = pl.BlockSpec(memory_space=pltpu.HBM)
    dma = pltpu.SemaphoreType.DMA
    held = pltpu.VMEM((depth, rows, cols), F32)
    field = jax.ShapeDtypeStruct((depth, rows, cols), F32)
    columns = nspace // 2
    most = max(W * (columns - 1) // columns, 1)
    gradient, first, second, total = pl.pallas_call(
        functools.partial(kernel, nshot, nspace),
        out_shape=(
            pltpu.VMEM((depth, yq, cols), F32),
            held,
            held,
            pltpu.VMEM((8, 128), F32),
        ),
        in_specs=[anyspace] * 9,
        out_specs=(vmem, vmem, vmem, vmem),
        scratch_shapes=[
            pltpu.SMEM(receiver_cell.shape, jnp.int32),
            pltpu.SMEM(source_cell.shape, jnp.int32),
            pltpu.SMEM(scale_table.shape, F32),
            pltpu.SMEM(observed.shape[1:], F32),
            pltpu.VMEM(scale_index.shape[1:], jnp.int32),
            pltpu.VMEM(receiver_cell.shape, jnp.int32),
            pltpu.VMEM((ITERS + 2, depth + 2 * W, rows, cols), F32),
            pltpu.VMEM((ITERS - 1, depth, rows, cols), F32),
            pltpu.VMEM((depth, rows, cols), F32),
            pltpu.VMEM((levels, depth, rows, QBLOCK), jnp.int32),
            pltpu.VMEM((128 // depth, depth, rows * blocks), F32),
            pltpu.VMEM((blocks, rows, 128), F32),
            pltpu.VMEM((nrec, 128), jnp.int32),
            pltpu.VMEM((ITERS, nrec, 128), F32),
            pltpu.VMEM((depth, rows, cols), F32),
            pltpu.VMEM((pairs, depth, yq, cols), F32),
            pltpu.VMEM((pairs, depth, yq, cols), F32),
            pltpu.VMEM((max(pairs - 1, 1), depth, yq, cols), F32),
            pltpu.VMEM((depth, rows, nrec), BF16),
            pltpu.VMEM((ITERS, nrec, cols), BF16),
            pltpu.VMEM((ITERS, nrec, cols), BF16),
            pltpu.VMEM((cols, cols), BF16),
            pltpu.VMEM((cols, cols), BF16),
            pltpu.VMEM((ITERS, nrec, QBLOCK), jnp.int32),
            pltpu.VMEM((ITERS, nrec, rows * blocks), F32),
            pltpu.VMEM((nshot, 8, 128), F32),
            pltpu.VMEM((8, 128), F32),
            pltpu.VMEM((8, 128), F32),
            pltpu.VMEM((8, 128), F32),
            pltpu.VMEM((2, columns, 8, 128), F32),
            pltpu.VMEM((2, columns, 8, 128), F32),
            pltpu.VMEM((ITERS, NC, most, rows // NC, cols), F32),
            dma((2, ITERS, NC)),
            dma((2, ITERS, NC)),
            dma((ITERS, NC, most)),
            dma((ITERS, NC, most)),
            dma((pairs, 3)),
            dma((pairs, 3)),
            dma((max(pairs - 1, 1), 3)),
            dma((max(pairs - 1, 1), 3)),
            dma((nshot - 1,)),
            dma((nshot - 1,)),
            dma((2,)),
            dma((2,)),
            dma((2,)),
            dma((6,)),
            dma((6,)),
        ],
        compiler_params=pltpu.CompilerParams(
            collective_id=0, has_side_effects=True, vmem_limit_bytes=52000000
        ),
    )(
        receiver_cell,
        source_cell,
        scale_table,
        observed[0],
        adjoint_now[0],
        adjoint_later[0],
        courant,
        checkpoint_codes[0],
        scale_index[0],
    )
    count = nshot * ITERS * nrec * nspace
    gradient, first, second, misfit = pl.pallas_call(
        functools.partial(finish, 0.5 / count),
        out_shape=(jax.ShapeDtypeStruct(gradient.shape, F32), field, field, jax.ShapeDtypeStruct((1, 1), F32)),
        in_specs=[vmem] * 4,
        out_specs=(anyspace, anyspace, anyspace, vmem),
        scratch_shapes=[dma((3,))],
        compiler_params=pltpu.CompilerParams(vmem_limit_bytes=16000000),
    )(gradient, first, second, total)
    return (gradient, first[None], second[None], misfit.reshape(()))


def solution(mesh):
    placed = (
        P("shot", "space", None, None),
        P("shot", "space", None, None),
        P("space", None, None),
        P("shot", None, "space", None, None),
        P("shot", None, "space", None),
        P(),
        P("shot", "space"),
        P("shot", None, "space"),
        P("shot", None),
    )
    return jax.shard_map(
        functools.partial(body, mesh.shape["shot"], mesh.shape["space"]),
        mesh=mesh,
        in_specs=placed,
        out_specs=(
            P("space", "shot", None),
            P("shot", "space", None, None),
            P("shot", "space", None, None),
            P(),
        ),
        check_vma=False,
    )
```

```python
import functools

import jax
import jax.numpy as jnp
from jax import lax
from jax.experimental import pallas as pl
from jax.experimental.pallas import tpu as pltpu
from jax.sharding import PartitionSpec as P

ITERS = 4
QBLOCK = 128
MUTE = 8
W = 4
NC = 2
F32 = jnp.float32
BF16 = jnp.bfloat16
MESH = pl.DeviceIdType.MESH

COEFFS = (-205.0 / 72.0, 8.0 / 5.0, -1.0 / 5.0, 8.0 / 315.0, -1.0 / 560.0)


def split(value):
    high = value.astype(BF16)
    return high, (value - high.astype(F32)).astype(BF16)


def dot(a, b):
    return jnp.dot(a, b, preferred_element_type=F32)


def band(rows, cols, first):
    i = first + lax.broadcasted_iota(jnp.int32, (rows, cols), 0)
    j = lax.broadcasted_iota(jnp.int32, (rows, cols), 1)
    d = jnp.abs(i - j)
    value = jnp.zeros((rows, cols), F32)
    for k in range(1, 5):
        value = jnp.where(d == k, COEFFS[k], value)
    return split(value)


def kernel(
    nshot,
    nspace,
    cells_h,
    source_h,
    table_h,
    observed_h,
    now_h,
    later_h,
    cour_h,
    words_h,
    index_h,
    grad,
    first,
    second,
    misfit,
    cells_s,
    source_s,
    table,
    observed,
    index,
    cells_row,
    E,
    D,
    cour,
    words,
    SC,
    TS,
    PC,
    OB,
    IM,
    RA,
    S,
    RB,
    PR,
    QH,
    QL,
    CH,
    CL,
    GW,
    GS,
    MB,
    MT,
    ST,
    PX,
    CO,
    CI,
    RL,
    halo_send,
    halo_recv,
    relay_recv,
    relay_send,
    a_send,
    a_recv,
    b_send,
    b_recv,
    m_sem,
    p_sem,
    s_send,
    s_recv,
    small_sem,
    local_sem,
):
    depth, rows, cols = cour.shape
    nrec = cells_row.shape[1]
    blocks = cols // QBLOCK
    ych = rows // NC
    shot = lax.axis_index("shot")
    space = lax.axis_index("space")
    has_low = space > 0
    has_high = space < nspace - 1

    barrier = pltpu.get_barrier_semaphore()
    near = ((-2, space >= 2), (-1, has_low), (1, has_high), (2, space < nspace - 2))
    for d, there in near:

        @pl.when(there)
        def _():
            pl.semaphore_signal(
                barrier, inc=1, device_id={"space": space + d}, device_id_type=MESH
            )

    for d in range(1, nshot):
        pl.semaphore_signal(
            barrier, inc=1, device_id={"shot": lax.rem(shot + d, nshot)}, device_id_type=MESH
        )

    edge_low = pltpu.make_async_copy(
        now_h.at[pl.ds(0, W)], E.at[1, pl.ds(W, W)], local_sem.at[4]
    )
    edge_high = pltpu.make_async_copy(
        now_h.at[pl.ds(depth - W, W)], E.at[1, pl.ds(depth, W)], local_sem.at[4]
    )
    inner = depth - 2 * W
    in_now = pltpu.make_async_copy(
        now_h.at[pl.ds(W, inner)], E.at[1, pl.ds(2 * W, inner)], local_sem.at[0]
    )
    in_later = pltpu.make_async_copy(later_h, E.at[0, pl.ds(W, depth)], local_sem.at[1])
    in_cour = pltpu.make_async_copy(cour_h, cour, local_sem.at[2])
    in_words = pltpu.make_async_copy(words_h, words, local_sem.at[3])
    edge_low.start()
    edge_high.start()
    in_words.start()
    in_now.start()
    in_cour.start()
    in_later.start()
    small = [
        pltpu.make_async_copy(source, target, small_sem.at[n])
        for n, (source, target) in enumerate(
            (
                (index_h, index),
                (cells_h, cells_row),
                (cells_h, cells_s),
                (source_h, source_s),
                (table_h, table),
                (observed_h, observed),
            )
        )
    ]
    for copy in small:
        copy.start()

    pltpu.make_async_copy(
        now_h.at[pl.ds(0, 2 * W)], E.at[1, pl.ds(W, 2 * W)], local_sem.at[4]
    ).wait()
    present = sum(there.astype(jnp.int32) for _, there in near)
    pl.semaphore_wait(barrier, nshot - 1 + present)

    odd = lax.rem(space, 2)
    column = space // 2
    columns = nspace // 2
    lean = W * (columns - 1 - column) // columns
    full = W * column // columns
    n_out = jnp.where(odd == 1, lean, full)
    n_in = jnp.where(odd == 1, full, lean)

    def eased(count, side, t, c):
        if c != NC - 1:
            return count
        early = jnp.logical_and(odd == side, jnp.logical_and(column == 0, lax.rem(shot, 2) == 0))
        early = jnp.logical_and(early, t == ITERS - 1)
        return jnp.where(early, jnp.maximum(count - 1, 0), count)

    most = RL.shape[2]

    def rows_of(c):
        return pl.ds(c * ych, ych)

    def halo(t, c, p, up, planes=1):
        src_z = depth + p if up else W + p
        dst_z = p if up else W + depth + p
        return pltpu.make_async_remote_copy(
            src_ref=E.at[t + 1, pl.ds(src_z, planes), rows_of(c), :],
            dst_ref=E.at[t + 1, pl.ds(dst_z, planes), rows_of(c), :],
            send_sem=halo_send.at[int(up), t % 2, c],
            recv_sem=halo_recv.at[int(up), t % 2, c],
            device_id={"space": space + (1 if up else -1)},
            device_id_type=MESH,
        )

    def detour(t, c, p):
        return pltpu.make_async_remote_copy(
            src_ref=E.at[t + 1, W + p + odd * (depth - W), rows_of(c), :],
            dst_ref=RL.at[t, c, p],
            send_sem=halo_send.at[odd, t % 2, c],
            recv_sem=relay_recv.at[t % 2, c, p],
            device_id={"space": space + 1 - 2 * odd},
            device_id_type=MESH,
        )

    def onward(t, c, p, planes=1):
        return pltpu.make_async_remote_copy(
            src_ref=RL.at[t, c, pl.ds(p, planes)],
            dst_ref=E.at[t + 1, pl.ds(p + odd * (W + depth), planes), rows_of(c), :],
            send_sem=relay_send.at[t % 2, c],
            recv_sem=halo_recv.at[1 - odd, t % 2, c],
            device_id={"space": space + 2 - 4 * odd},
            device_id_type=MESH,
        )

    def send(t, c):
        out = eased(n_out, 1, t, c)
        for p in range(most):

            @pl.when(p < out)
            def _():
                detour(t, c, p).start()

        for p in range(W):

            @pl.when(jnp.logical_and(has_high, p >= odd * out))
            def _():
                halo(t, c, p, True).start()

            @pl.when(jnp.logical_and(has_low, p >= (1 - odd) * out))
            def _():
                halo(t, c, p, False).start()

    def relay(t, c):
        n = eased(n_in, 0, t, c)
        for p in range(most):

            @pl.when(p < n)
            def _():
                detour(t, c, p).wait_recv()
                onward(t, c, p).start()

    def drain(t, c):
        @pl.when(has_high)
        def _():
            halo(t, c, 0, True, W).wait_send()

        @pl.when(has_low)
        def _():
            halo(t, c, 0, False, W).wait_send()

        n = eased(n_in, 0, t, c)
        for count in range(1, most + 1):

            @pl.when(n == count)
            def _():
                onward(t, c, 0, count).wait_send()

    for c in range(NC):
        send(0, c)

    @pl.loop(0, cols // 64)
    def _(i):
        start = pl.multiple_of(i * 64, 64)
        high, low = band(64, cols, start)
        CH[pl.ds(start, 64), :] = high
        CL[pl.ds(start, 64), :] = low

    yh, yl = band(rows, rows, 0)
    for copy in small:
        copy.wait()

    entry = index[...]
    scale = jnp.zeros(entry.shape, F32)
    for e in range(table.shape[0]):
        scale = jnp.where(entry == e, table[e], scale)
    levels = entry.shape[0]
    SC[0:levels] = scale
    SC[levels:] = jnp.zeros((SC.shape[0] - levels,) + entry.shape[1:], F32)

    slab = depth * rows * cols
    in_words.wait()

    @pl.loop(0, nrec, unroll=4)
    def _(r):
        cell = lax.rem(cells_s[0, r], slab)
        row = cell // cols
        z = row // rows
        y = lax.rem(row, rows)
        for k in range(1, ITERS + 1):
            GW[k - 1, pl.ds(r, 1), :] = words[k, z, pl.ds(y, 1), :]
            GS[k - 1, pl.ds(r, 1), :] = SC[k, pl.ds(z, 1), :]
            OB[k - 1, pl.ds(r, 1), :] = jnp.full((1, 128), observed[k - 1, r], F32)
        PC[pl.ds(r, 1), :] = jnp.full((1, 128), cell - z * (rows * cols), jnp.int32)

    place = PC[:, 0:1]
    xcol = lax.rem(place, cols)
    mcol = xcol // QBLOCK
    jcol = lax.rem(xcol, QBLOCK)
    scol = place // cols * blocks + mcol
    lane = lax.broadcasted_iota(jnp.int32, (nrec, QBLOCK), 1)
    sl = lax.broadcasted_iota(jnp.int32, (nrec, rows * blocks), 1)
    xl = lax.broadcasted_iota(jnp.int32, (nrec, cols), 1)
    squares = jnp.zeros((1, 1), F32)
    for k in range(1, ITERS + 1):
        code = jnp.bitwise_and(jnp.right_shift(GW[k - 1], 8 * mcol), 255) - 128
        code = jnp.sum(jnp.where(lane == jcol, code.astype(F32), 0.0), axis=1, keepdims=True)
        scale = jnp.sum(jnp.where(sl == scol, GS[k - 1], 0.0), axis=1, keepdims=True)
        residual = code * scale - OB[k - 1, :, 0:1]
        squares = squares + jnp.sum(residual * residual, axis=0, keepdims=True)
        high, low = split(jnp.where(xl == xcol, residual, 0.0))
        QH[ITERS - k] = high
        QL[ITERS - k] = low
    crow = lax.rem(cells_row[...], slab) // cols
    for z in range(depth):
        i = z * rows + lax.broadcasted_iota(jnp.int32, (rows, nrec), 0)
        PR[z] = jnp.where(i == crow, 1.0, 0.0).astype(BF16)

    tile = jnp.broadcast_to(squares, (8, 128))
    MT[...] = tile
    MB[pl.ds(shot, 1)] = tile.reshape(1, 8, 128)

    def misfit_copy(d):
        return pltpu.make_async_remote_copy(
            src_ref=MT,
            dst_ref=MB.at[shot],
            send_sem=m_sem.at[0],
            recv_sem=m_sem.at[1],
            device_id={"shot": lax.rem(shot + d, nshot)},
            device_id_type=MESH,
        )

    def pair_copy():
        return pltpu.make_async_remote_copy(
            src_ref=ST,
            dst_ref=PX,
            send_sem=p_sem.at[0],
            recv_sem=p_sem.at[1],
            device_id={"space": space + 1 - 2 * odd},
            device_id_type=MESH,
        )

    def chain_copy(way):
        return pltpu.make_async_remote_copy(
            src_ref=CO.at[way],
            dst_ref=CI.at[way],
            send_sem=s_send.at[way],
            recv_sem=s_recv.at[way],
            device_id={"space": space + (2 if way else -2)},
            device_id_type=MESH,
        )

    def chain(slot):
        for way in (0, 1):
            place = column if way else columns - 1 - column
            turn = jnp.logical_or(place == slot, jnp.logical_and(slot == 3, place > slot))

            @pl.when(turn)
            def _():
                @pl.when(place > 0)
                def _():
                    chain_copy(way).wait_recv()
                    CO[way] = CI[way]

                CO[way, pl.ds(column, 1)] = (ST[...] + PX[...]).reshape(1, 8, 128)

                @pl.when(place < columns - 1)
                def _():
                    chain_copy(way).start()

    for d in range(1, nshot):
        misfit_copy(d).start()

    relay(0, 0)
    in_now.wait()
    in_later.wait()
    in_cour.wait()

    groups = (0, depth // W - 1) + tuple(range(1, depth // W - 1))

    def local(t, chosen):
        for g in chosen:
            z0 = g * W
            u = E[t + 1, W + z0 : W + z0 + W].reshape(W * rows, cols)
            uh, ul = split(u)
            lap = dot(uh, CH[...]) + dot(ul, CH[...]) + dot(uh, CL[...])
            for j in range(W):
                z = z0 + j
                part = slice(j * rows, (j + 1) * rows)
                up = u[part]
                acc = lap[part] + (3.0 * COEFFS[0]) * up
                acc = acc + dot(yh, uh[part]) + dot(yh, ul[part]) + dot(yl, uh[part])
                for i in range(1, 5):
                    if z + i < depth:
                        acc = acc + COEFFS[i] * E[t + 1, W + z + i]
                    if z - i >= 0:
                        acc = acc + COEFFS[i] * E[t + 1, W + z - i]
                inject = dot(PR[z], QH[t]) + dot(PR[z], QL[t])
                E[t + 2, W + z] = 2.0 * up - E[t, W + z] + cour[z] * acc + inject

    def spread():
        i = lax.broadcasted_iota(jnp.int32, (rows, rows * blocks), 0)
        j = lax.broadcasted_iota(jnp.int32, (rows, rows * blocks), 1)
        flat = SC[...].reshape(128, rows * blocks)
        high = flat.astype(BF16)
        rest = flat - high.astype(F32)
        pieces = (high,) + split(rest)
        for m in range(blocks):
            pick = jnp.where(j == blocks * i + m, 1.0, 0.0).astype(BF16)
            moved = jnp.zeros((rows, 128), F32)
            for piece in pieces:
                moved = moved + lax.dot_general(
                    pick, piece, (((1,), (1,)), ((), ())), preferred_element_type=F32
                )
            TS[m] = moved

    def decode(part):
        @pl.loop(0, depth // 4)
        def _(step):
            z = part * (depth // 4) + step
            for m in range(blocks):
                xs = slice(m * QBLOCK, (m + 1) * QBLOCK)
                scale = pltpu.roll(TS[m], lax.rem(128 - z, 128), 1)
                f = []
                for k in range(ITERS + 2):
                    code = jnp.bitwise_and(jnp.right_shift(words[k, z], 8 * m), 255) - 128
                    f.append(code.astype(F32) * scale[:, k * depth : k * depth + 1])
                for t in range(ITERS):
                    k = ITERS - t
                    diff = f[k + 1] - 2.0 * f[k] + f[k - 1]
                    if t == 0:
                        IM[z, :, xs] = E[1, W + z, :, xs] * diff
                    else:
                        D[t - 1, z, :, xs] = diff

    spread()
    local(0, groups)

    pltpu.make_async_remote_copy(
        src_ref=MB.at[pl.ds(0, nshot - 1)],
        dst_ref=MB.at[pl.ds(0, nshot - 1)],
        send_sem=m_sem.at[0],
        recv_sem=m_sem.at[1],
        device_id={"shot": lax.rem(shot + 1, nshot)},
        device_id_type=MESH,
    ).wait()
    total = MB[0]
    for d in range(1, nshot):
        total = total + MB[d]
    ST[...] = total
    pair_copy().start()
    CO[...] = jnp.zeros(CO.shape, F32)

    def fix(t, c, target, base):
        ys = rows_of(c)

        @pl.when(has_low)
        def _():
            halo(t, c, 0, True, W).wait_recv()
            for j in range(W):
                acc = COEFFS[j + 1] * E[t + 1, W - 1, ys, :]
                for i in range(j + 2, 5):
                    acc = acc + COEFFS[i] * E[t + 1, W + j - i, ys, :]
                target[base + j, ys, :] += cour[j, ys, :] * acc

        @pl.when(has_high)
        def _():
            halo(t, c, 0, False, W).wait_recv()
            for j in range(W):
                z = depth - 1 - j
                acc = COEFFS[j + 1] * E[t + 1, W + depth, ys, :]
                for i in range(j + 2, 5):
                    acc = acc + COEFFS[i] * E[t + 1, W + z + i, ys, :]
                target[base + z, ys, :] += cour[z, ys, :] * acc

    first_z = space * depth
    core = lax.rem(shot, 2)
    pair = shot // 2
    pairs = nshot // 2
    yq = rows // nshot
    pieces = (((W, inner),), ((0, W), (depth - W, W)))

    def quarter(index):
        return pl.ds(pl.multiple_of(index * yq, yq), yq)

    def mute(z):
        dz = first_z + z - source_s[0, 0]
        dy = lax.broadcasted_iota(jnp.int32, (rows, cols), 0) - source_s[0, 1]
        dx = lax.broadcasted_iota(jnp.int32, (rows, cols), 1) - source_s[0, 2]
        dist = (dz * dz + dy * dy + dx * dx).astype(F32)
        IM[z] = IM[z] * (1.0 - jnp.exp(dist * (-1.0 / (2.0 * MUTE * MUTE))))

    def copy_a(source, target, n):
        return pltpu.make_async_remote_copy(
            src_ref=source,
            dst_ref=target,
            send_sem=a_send.at[n],
            recv_sem=a_recv.at[n],
            device_id={"shot": shot + 1 - 2 * core},
            device_id_type=MESH,
        )

    def copy_b(d, n, at):
        other = lax.rem(pair + d, pairs)
        return pltpu.make_async_remote_copy(
            src_ref=S.at[other, at],
            dst_ref=RB.at[d - 1, at],
            send_sem=b_send.at[d - 1, n],
            recv_sem=b_recv.at[d - 1, n],
            device_id={"shot": 2 * other + core},
            device_id_type=MESH,
        )

    def whole_of(n):
        return pl.ds(0, sum(count for _, count in pieces[n]))

    def offer(n):
        for piece in pieces[n]:
            at = pl.ds(*piece)
            for h in range(pairs):
                copy_a(IM.at[at, quarter(2 * h + 1 - core), :], RA.at[h, at], n).start()

    def pass_on(n):
        copy_a(S.at[:, whole_of(n)], RA.at[:, whole_of(n)], n).wait()
        for piece in pieces[n]:
            at = pl.ds(*piece)
            for h in range(pairs):
                S[h, at] = IM[at, quarter(2 * h + core), :] + RA[h, at]
            for d in range(1, pairs):
                copy_b(d, n, at).start()

    @pl.loop(0, ITERS - 1)
    def _(t):
        fix(t, 0, E.at[t + 2], W)
        send(t + 1, 0)

        @pl.when(t == 1)
        def _():
            pair_copy().wait()

        @pl.when(t > 0)
        def _():
            chain(2 * t - 2)

        @pl.when(t < 2)
        def _():
            decode(2 * t)

        relay(t, 1)

        @pl.when(t < 2)
        def _():
            decode(2 * t + 1)

        @pl.when(t == ITERS - 2)
        def _():
            pass_on(0)

        fix(t, 1, E.at[t + 2], W)
        send(t + 1, 1)

        @pl.when(t == ITERS - 2)
        def _():
            for low in (0, depth - W):

                @pl.loop(low, low + W)
                def _(z):
                    IM[z] = IM[z] + E[ITERS, W + z] * D[ITERS - 2, z]
                    mute(z)

            offer(1)

        local(t + 1, groups[:2])
        relay(t + 1, 0)

        @pl.when(t == ITERS - 2)
        def _():
            pass_on(1)

        local(t + 1, groups[2:])

        @pl.when(t > 0)
        def _():
            chain(2 * t - 1)

        drain(t, 0)
        drain(t, 1)

        @pl.when(t == ITERS - 3)
        def _():
            @pl.loop(0, depth)
            def _(z):
                value = IM[z]
                for k in range(ITERS - 2):
                    value = value + E[k + 2, W + z] * D[k, z]
                IM[z] = value

            @pl.loop(W, depth - W)
            def _(z):
                IM[z] = IM[z] + E[ITERS, W + z] * D[ITERS - 2, z]
                mute(z)

            offer(0)

    @pl.loop(0, depth)
    def _(z):
        second[z] = E[ITERS, W + z]
        first[z] = E[ITERS + 1, W + z]

    fix(ITERS - 1, 0, first, 0)
    relay(ITERS - 1, 1)
    drain(ITERS - 1, 0)
    total = S[pair]
    for d in range(1, pairs):
        for n in range(len(pieces)):
            copy_b(d, n, whole_of(n)).wait()
        total = total + RB[d - 1]
    grad[...] = total

    whole = jnp.zeros((8, 128), F32)
    for way in (0, 1):
        @pl.when(column != (columns - 1 if way else 0))
        def _():
            chain_copy(way).wait_send()

    @pl.when(column < columns - 1)
    def _():
        CO[1] = CO[1] + CI[0]

    for k in range(columns):
        whole = whole + CO[1, k]
    misfit[...] = whole

    fix(ITERS - 1, 1, first, 0)

    drain(ITERS - 1, 1)


def finish(factor, grad, first, second, total, grad_o, first_o, second_o, misfit, sem):
    copies = [
        pltpu.make_async_copy(source, target, sem.at[n])
        for n, (source, target) in enumerate(((first, first_o), (second, second_o), (grad, grad_o)))
    ]
    for copy in copies:
        copy.start()
    misfit[...] = total[0:1, 0:1] * factor
    for copy in copies:
        copy.wait()


def body(
    nshot,
    nspace,
    adjoint_now,
    adjoint_later,
    courant,
    checkpoint_codes,
    scale_index,
    scale_table,
    receiver_cell,
    observed,
    source_cell,
):
    depth, rows, cols = courant.shape
    levels = checkpoint_codes.shape[1]
    nrec = receiver_cell.shape[1]
    blocks = cols // QBLOCK
    pairs = nshot // 2
    yq = rows // nshot
    vmem = pl.BlockSpec(memory_space=pltpu.VMEM)
    anyspace = pl.BlockSpec(memory_space=pltpu.HBM)
    dma = pltpu.SemaphoreType.DMA
    held = pltpu.VMEM((depth, rows, cols), F32)
    field = jax.ShapeDtypeStruct((depth, rows, cols), F32)
    columns = nspace // 2
    most = max(W * (columns - 1) // columns, 1)
    gradient, first, second, total = pl.pallas_call(
        functools.partial(kernel, nshot, nspace),
        out_shape=(
            pltpu.VMEM((depth, yq, cols), F32),
            held,
            held,
            pltpu.VMEM((8, 128), F32),
        ),
        in_specs=[anyspace] * 9,
        out_specs=(vmem, vmem, vmem, vmem),
        scratch_shapes=[
            pltpu.SMEM(receiver_cell.shape, jnp.int32),
            pltpu.SMEM(source_cell.shape, jnp.int32),
            pltpu.SMEM(scale_table.shape, F32),
            pltpu.SMEM(observed.shape[1:], F32),
            pltpu.VMEM(scale_index.shape[1:], jnp.int32),
            pltpu.VMEM(receiver_cell.shape, jnp.int32),
            pltpu.VMEM((ITERS + 2, depth + 2 * W, rows, cols), F32),
            pltpu.VMEM((ITERS - 1, depth, rows, cols), F32),
            pltpu.VMEM((depth, rows, cols), F32),
            pltpu.VMEM((levels, depth, rows, QBLOCK), jnp.int32),
            pltpu.VMEM((128 // depth, depth, rows * blocks), F32),
            pltpu.VMEM((blocks, rows, 128), F32),
            pltpu.VMEM((nrec, 128), jnp.int32),
            pltpu.VMEM((ITERS, nrec, 128), F32),
            pltpu.VMEM((depth, rows, cols), F32),
            pltpu.VMEM((pairs, depth, yq, cols), F32),
            pltpu.VMEM((pairs, depth, yq, cols), F32),
            pltpu.VMEM((max(pairs - 1, 1), depth, yq, cols), F32),
            pltpu.VMEM((depth, rows, nrec), BF16),
            pltpu.VMEM((ITERS, nrec, cols), BF16),
            pltpu.VMEM((ITERS, nrec, cols), BF16),
            pltpu.VMEM((cols, cols), BF16),
            pltpu.VMEM((cols, cols), BF16),
            pltpu.VMEM((ITERS, nrec, QBLOCK), jnp.int32),
            pltpu.VMEM((ITERS, nrec, rows * blocks), F32),
            pltpu.VMEM((nshot, 8, 128), F32),
            pltpu.VMEM((8, 128), F32),
            pltpu.VMEM((8, 128), F32),
            pltpu.VMEM((8, 128), F32),
            pltpu.VMEM((2, columns, 8, 128), F32),
            pltpu.VMEM((2, columns, 8, 128), F32),
            pltpu.VMEM((ITERS, NC, most, rows // NC, cols), F32),
            dma((2, 2, NC)),
            dma((2, 2, NC)),
            dma((2, NC, most)),
            dma((2, NC)),
            dma((2,)),
            dma((2,)),
            dma((max(pairs - 1, 1), 2)),
            dma((max(pairs - 1, 1), 2)),
            dma((2,)),
            dma((2,)),
            dma((2,)),
            dma((2,)),
            dma((6,)),
            dma((5,)),
        ],
        compiler_params=pltpu.CompilerParams(
            collective_id=0, has_side_effects=True, vmem_limit_bytes=52000000
        ),
    )(
        receiver_cell,
        source_cell,
        scale_table,
        observed[0],
        adjoint_now[0],
        adjoint_later[0],
        courant,
        checkpoint_codes[0],
        scale_index[0],
    )
    count = nshot * ITERS * nrec * nspace
    gradient, first, second, misfit = pl.pallas_call(
        functools.partial(finish, 0.5 / count),
        out_shape=(jax.ShapeDtypeStruct(gradient.shape, F32), field, field, jax.ShapeDtypeStruct((1, 1), F32)),
        in_specs=[vmem] * 4,
        out_specs=(anyspace, anyspace, anyspace, vmem),
        scratch_shapes=[dma((3,))],
        compiler_params=pltpu.CompilerParams(vmem_limit_bytes=16000000),
    )(gradient, first, second, total)
    return (gradient, first[None], second[None], misfit.reshape(()))


def solution(mesh):
    placed = (
        P("shot", "space", None, None),
        P("shot", "space", None, None),
        P("space", None, None),
        P("shot", None, "space", None, None),
        P("shot", None, "space", None),
        P(),
        P("shot", "space"),
        P("shot", None, "space"),
        P("shot", None),
    )
    return jax.shard_map(
        functools.partial(body, mesh.shape["shot"], mesh.shape["space"]),
        mesh=mesh,
        in_specs=placed,
        out_specs=(
            P("space", "shot", None),
            P("shot", "space", None, None),
            P("shot", "space", None, None),
            P(),
        ),
        check_vma=False,
    )
```

```python
import functools

import jax
import jax.numpy as jnp
from jax import lax
from jax.experimental import pallas as pl
from jax.experimental.pallas import tpu as pltpu
from jax.sharding import PartitionSpec as P

ITERS = 4
QBLOCK = 128
MUTE = 8
W = 4
NC = 2
F32 = jnp.float32
BF16 = jnp.bfloat16
MESH = pl.DeviceIdType.MESH

COEFFS = (-205.0 / 72.0, 8.0 / 5.0, -1.0 / 5.0, 8.0 / 315.0, -1.0 / 560.0)


def split(value):
    high = value.astype(BF16)
    return high, (value - high.astype(F32)).astype(BF16)


def dot(a, b):
    return jnp.dot(a, b, preferred_element_type=F32)


def band(rows, cols, first):
    i = first + lax.broadcasted_iota(jnp.int32, (rows, cols), 0)
    j = lax.broadcasted_iota(jnp.int32, (rows, cols), 1)
    d = jnp.abs(i - j)
    value = jnp.zeros((rows, cols), F32)
    for k in range(1, 5):
        value = jnp.where(d == k, COEFFS[k], value)
    return split(value)


def kernel(
    nshot,
    nspace,
    cells_h,
    source_h,
    table_h,
    observed_h,
    now_h,
    later_h,
    cour_h,
    words_h,
    index_h,
    grad,
    first,
    second,
    misfit,
    cells_s,
    source_s,
    table,
    observed,
    index,
    cells_row,
    E,
    D,
    cour,
    words,
    SC,
    TS,
    PC,
    OB,
    IM,
    RA,
    S,
    RB,
    PR,
    QH,
    QL,
    CH,
    CL,
    GW,
    GS,
    MB,
    MT,
    ST,
    PX,
    CO,
    CI,
    RL,
    halo_send,
    halo_recv,
    relay_recv,
    relay_send,
    a_send,
    a_recv,
    b_send,
    b_recv,
    m_sem,
    p_sem,
    s_send,
    s_recv,
    small_sem,
    local_sem,
    ready,
):
    depth, rows, cols = cour.shape
    nrec = cells_row.shape[1]
    blocks = cols // QBLOCK
    ych = rows // NC
    shot = lax.axis_index("shot")
    space = lax.axis_index("space")
    has_low = space > 0
    has_high = space < nspace - 1

    barrier = pltpu.get_barrier_semaphore()
    odd = lax.rem(space, 2)
    has_under = space >= 2
    has_over = space < nspace - 2
    pl.semaphore_signal(
        barrier, inc=1, device_id={"space": space + 1 - 2 * odd}, device_id_type=MESH
    )
    near = ((-2, has_under), (2, has_over))
    for d, there in near:

        @pl.when(there)
        def _():
            pl.semaphore_signal(
                barrier, inc=1, device_id={"space": space + d}, device_id_type=MESH
            )

    for d in range(1, nshot):
        pl.semaphore_signal(
            barrier, inc=1, device_id={"shot": lax.rem(shot + d, nshot)}, device_id_type=MESH
        )

    edges = [
        pltpu.make_async_copy(
            now_h.at[pl.ds(z, W), pl.ds(c * ych, ych)],
            E.at[1, pl.ds(W + z, W), pl.ds(c * ych, ych)],
            local_sem.at[4 + c],
        )
        for c in range(NC)
        for z in (0, depth - W)
    ]
    inner = depth - 2 * W
    in_now = pltpu.make_async_copy(
        now_h.at[pl.ds(W, inner)], E.at[1, pl.ds(2 * W, inner)], local_sem.at[0]
    )
    in_later = pltpu.make_async_copy(later_h, E.at[0, pl.ds(W, depth)], local_sem.at[1])
    in_cour = pltpu.make_async_copy(cour_h, cour, local_sem.at[2])
    in_words = pltpu.make_async_copy(words_h, words, local_sem.at[3])
    for copy in edges:
        copy.start()
    in_words.start()
    in_now.start()
    in_cour.start()
    in_later.start()
    small = [
        pltpu.make_async_copy(source, target, small_sem.at[n])
        for n, (source, target) in enumerate(
            (
                (index_h, index),
                (cells_h, cells_row),
                (cells_h, cells_s),
                (source_h, source_s),
                (table_h, table),
                (observed_h, observed),
            )
        )
    ]
    for copy in small:
        copy.start()

    present = sum(there.astype(jnp.int32) for _, there in near)
    pl.semaphore_wait(barrier, nshot + present)
    vouch = jnp.where(odd == 1, has_under, has_over)
    await_vouch = jnp.where(odd == 1, has_over, has_under)

    @pl.when(vouch)
    def _():
        pl.semaphore_signal(
            ready, inc=1, device_id={"space": space + 2 - 4 * odd}, device_id_type=MESH
        )


    column = space // 2
    columns = nspace // 2
    lean = W * (columns - 1 - column) // columns
    full = W * column // columns
    n_out = jnp.where(odd == 1, lean, full)
    n_in = jnp.where(odd == 1, full, lean)

    def eased(count, side, t, c):
        if c != NC - 1:
            return count
        early = jnp.logical_and(odd == side, jnp.logical_and(column == 0, lax.rem(shot, 2) == 0))
        early = jnp.logical_and(early, t == ITERS - 1)
        return jnp.where(early, jnp.maximum(count - 1, 0), count)

    most = RL.shape[2]

    def rows_of(c):
        return pl.ds(c * ych, ych)

    def halo(t, c, p, up, planes=1):
        src_z = depth + p if up else W + p
        dst_z = p if up else W + depth + p
        return pltpu.make_async_remote_copy(
            src_ref=E.at[t + 1, pl.ds(src_z, planes), rows_of(c), :],
            dst_ref=E.at[t + 1, pl.ds(dst_z, planes), rows_of(c), :],
            send_sem=halo_send.at[int(up), t % 2, c],
            recv_sem=halo_recv.at[int(up), t % 2, c],
            device_id={"space": space + (1 if up else -1)},
            device_id_type=MESH,
        )

    def detour(t, c, p):
        return pltpu.make_async_remote_copy(
            src_ref=E.at[t + 1, W + p + odd * (depth - W), rows_of(c), :],
            dst_ref=RL.at[t, c, p],
            send_sem=halo_send.at[odd, t % 2, c],
            recv_sem=relay_recv.at[t % 2, c, p],
            device_id={"space": space + 1 - 2 * odd},
            device_id_type=MESH,
        )

    def onward(t, c, p, planes=1):
        return pltpu.make_async_remote_copy(
            src_ref=RL.at[t, c, pl.ds(p, planes)],
            dst_ref=E.at[t + 1, pl.ds(p + odd * (W + depth), planes), rows_of(c), :],
            send_sem=relay_send.at[t % 2, c],
            recv_sem=halo_recv.at[1 - odd, t % 2, c],
            device_id={"space": space + 2 - 4 * odd},
            device_id_type=MESH,
        )

    def send_beside(t, c):
        out = eased(n_out, 1, t, c)
        for p in range(most):

            @pl.when(p < out)
            def _():
                detour(t, c, p).start()

        @pl.when(odd == 0)
        def _():
            halo(t, c, 0, True, W).start()

        @pl.when(odd == 1)
        def _():
            halo(t, c, 0, False, W).start()

    def send_across(t, c):
        out = eased(n_out, 1, t, c)
        for p in range(W):
            here = p >= out

            @pl.when(jnp.logical_and(here, jnp.logical_and(has_high, odd == 1)))
            def _():
                halo(t, c, p, True).start()

            @pl.when(jnp.logical_and(here, jnp.logical_and(has_low, odd == 0)))
            def _():
                halo(t, c, p, False).start()

    def send(t, c):
        send_beside(t, c)
        send_across(t, c)

    def relay(t, c):
        n = eased(n_in, 0, t, c)
        for p in range(most):

            @pl.when(p < n)
            def _():
                detour(t, c, p).wait_recv()
                onward(t, c, p).start()

    def drain(t, c):
        @pl.when(has_high)
        def _():
            halo(t, c, 0, True, W).wait_send()

        @pl.when(has_low)
        def _():
            halo(t, c, 0, False, W).wait_send()

        n = eased(n_in, 0, t, c)
        for count in range(1, most + 1):

            @pl.when(n == count)
            def _():
                onward(t, c, 0, count).wait_send()

    for c in range(NC):
        pltpu.make_async_copy(
            now_h.at[pl.ds(0, 2 * W), rows_of(c)],
            E.at[1, pl.ds(W, 2 * W), rows_of(c)],
            local_sem.at[4 + c],
        ).wait()
        send_beside(0, c)

    @pl.when(await_vouch)
    def _():
        pl.semaphore_wait(ready, 1)

    for c in range(NC):
        send_across(0, c)

    @pl.loop(0, cols // 64)
    def _(i):
        start = pl.multiple_of(i * 64, 64)
        high, low = band(64, cols, start)
        CH[pl.ds(start, 64), :] = high
        CL[pl.ds(start, 64), :] = low

    yh, yl = band(rows, rows, 0)
    for copy in small:
        copy.wait()

    entry = index[...]
    scale = jnp.zeros(entry.shape, F32)
    for e in range(table.shape[0]):
        scale = jnp.where(entry == e, table[e], scale)
    levels = entry.shape[0]
    SC[0:levels] = scale
    SC[levels:] = jnp.zeros((SC.shape[0] - levels,) + entry.shape[1:], F32)

    slab = depth * rows * cols
    in_words.wait()

    @pl.loop(0, nrec, unroll=4)
    def _(r):
        cell = lax.rem(cells_s[0, r], slab)
        row = cell // cols
        z = row // rows
        y = lax.rem(row, rows)
        for k in range(1, ITERS + 1):
            GW[k - 1, pl.ds(r, 1), :] = words[k, z, pl.ds(y, 1), :]
            GS[k - 1, pl.ds(r, 1), :] = SC[k, pl.ds(z, 1), :]
            OB[k - 1, pl.ds(r, 1), :] = jnp.full((1, 128), observed[k - 1, r], F32)
        PC[pl.ds(r, 1), :] = jnp.full((1, 128), cell - z * (rows * cols), jnp.int32)

    place = PC[:, 0:1]
    xcol = lax.rem(place, cols)
    mcol = xcol // QBLOCK
    jcol = lax.rem(xcol, QBLOCK)
    scol = place // cols * blocks + mcol
    lane = lax.broadcasted_iota(jnp.int32, (nrec, QBLOCK), 1)
    sl = lax.broadcasted_iota(jnp.int32, (nrec, rows * blocks), 1)
    xl = lax.broadcasted_iota(jnp.int32, (nrec, cols), 1)
    squares = jnp.zeros((1, 1), F32)
    for k in range(1, ITERS + 1):
        code = jnp.bitwise_and(jnp.right_shift(GW[k - 1], 8 * mcol), 255) - 128
        code = jnp.sum(jnp.where(lane == jcol, code.astype(F32), 0.0), axis=1, keepdims=True)
        scale = jnp.sum(jnp.where(sl == scol, GS[k - 1], 0.0), axis=1, keepdims=True)
        residual = code * scale - OB[k - 1, :, 0:1]
        squares = squares + jnp.sum(residual * residual, axis=0, keepdims=True)
        high, low = split(jnp.where(xl == xcol, residual, 0.0))
        QH[ITERS - k] = high
        QL[ITERS - k] = low
    crow = lax.rem(cells_row[...], slab) // cols
    for z in range(depth):
        i = z * rows + lax.broadcasted_iota(jnp.int32, (rows, nrec), 0)
        PR[z] = jnp.where(i == crow, 1.0, 0.0).astype(BF16)

    tile = jnp.broadcast_to(squares, (8, 128))
    MT[...] = tile
    MB[pl.ds(shot, 1)] = tile.reshape(1, 8, 128)

    def misfit_copy(d):
        return pltpu.make_async_remote_copy(
            src_ref=MT,
            dst_ref=MB.at[shot],
            send_sem=m_sem.at[0],
            recv_sem=m_sem.at[1],
            device_id={"shot": lax.rem(shot + d, nshot)},
            device_id_type=MESH,
        )

    def pair_copy():
        return pltpu.make_async_remote_copy(
            src_ref=ST,
            dst_ref=PX,
            send_sem=p_sem.at[0],
            recv_sem=p_sem.at[1],
            device_id={"space": space + 1 - 2 * odd},
            device_id_type=MESH,
        )

    def chain_copy(way):
        return pltpu.make_async_remote_copy(
            src_ref=CO.at[way],
            dst_ref=CI.at[way],
            send_sem=s_send.at[way],
            recv_sem=s_recv.at[way],
            device_id={"space": space + (2 if way else -2)},
            device_id_type=MESH,
        )

    def chain(slot):
        for way in (0, 1):
            place = column if way else columns - 1 - column
            turn = jnp.logical_or(place == slot, jnp.logical_and(slot == 3, place > slot))

            @pl.when(turn)
            def _():
                @pl.when(place > 0)
                def _():
                    chain_copy(way).wait_recv()
                    CO[way] = CI[way]

                CO[way, pl.ds(column, 1)] = (ST[...] + PX[...]).reshape(1, 8, 128)

                @pl.when(place < columns - 1)
                def _():
                    chain_copy(way).start()

    for d in range(1, nshot):
        misfit_copy(d).start()

    relay(0, 0)
    in_now.wait()
    in_later.wait()
    in_cour.wait()

    groups = (0, depth // W - 1) + tuple(range(1, depth // W - 1))

    def local(t, chosen):
        for g in chosen:
            z0 = g * W
            u = E[t + 1, W + z0 : W + z0 + W].reshape(W * rows, cols)
            uh, ul = split(u)
            lap = dot(uh, CH[...]) + dot(ul, CH[...]) + dot(uh, CL[...])
            for j in range(W):
                z = z0 + j
                part = slice(j * rows, (j + 1) * rows)
                up = u[part]
                acc = lap[part] + (3.0 * COEFFS[0]) * up
                acc = acc + dot(yh, uh[part]) + dot(yh, ul[part]) + dot(yl, uh[part])
                for i in range(1, 5):
                    if z + i < depth:
                        acc = acc + COEFFS[i] * E[t + 1, W + z + i]
                    if z - i >= 0:
                        acc = acc + COEFFS[i] * E[t + 1, W + z - i]
                inject = dot(PR[z], QH[t]) + dot(PR[z], QL[t])
                E[t + 2, W + z] = 2.0 * up - E[t, W + z] + cour[z] * acc + inject

    def spread():
        i = lax.broadcasted_iota(jnp.int32, (rows, rows * blocks), 0)
        j = lax.broadcasted_iota(jnp.int32, (rows, rows * blocks), 1)
        flat = SC[...].reshape(128, rows * blocks)
        high = flat.astype(BF16)
        rest = flat - high.astype(F32)
        pieces = (high,) + split(rest)
        for m in range(blocks):
            pick = jnp.where(j == blocks * i + m, 1.0, 0.0).astype(BF16)
            moved = jnp.zeros((rows, 128), F32)
            for piece in pieces:
                moved = moved + lax.dot_general(
                    pick, piece, (((1,), (1,)), ((), ())), preferred_element_type=F32
                )
            TS[m] = moved

    def decode(part):
        @pl.loop(0, depth // 4)
        def _(step):
            z = part * (depth // 4) + step
            for m in range(blocks):
                xs = slice(m * QBLOCK, (m + 1) * QBLOCK)
                scale = pltpu.roll(TS[m], lax.rem(128 - z, 128), 1)
                f = []
                for k in range(ITERS + 2):
                    code = jnp.bitwise_and(jnp.right_shift(words[k, z], 8 * m), 255) - 128
                    f.append(code.astype(F32) * scale[:, k * depth : k * depth + 1])
                for t in range(ITERS):
                    k = ITERS - t
                    diff = f[k + 1] - 2.0 * f[k] + f[k - 1]
                    if t == 0:
                        IM[z, :, xs] = E[1, W + z, :, xs] * diff
                    else:
                        D[t - 1, z, :, xs] = diff

    spread()
    local(0, groups)

    pltpu.make_async_remote_copy(
        src_ref=MB.at[pl.ds(0, nshot - 1)],
        dst_ref=MB.at[pl.ds(0, nshot - 1)],
        send_sem=m_sem.at[0],
        recv_sem=m_sem.at[1],
        device_id={"shot": lax.rem(shot + 1, nshot)},
        device_id_type=MESH,
    ).wait()
    total = MB[0]
    for d in range(1, nshot):
        total = total + MB[d]
    ST[...] = total
    pair_copy().start()
    CO[...] = jnp.zeros(CO.shape, F32)

    def fix(t, c, target, base):
        ys = rows_of(c)

        @pl.when(has_low)
        def _():
            halo(t, c, 0, True, W).wait_recv()
            for j in range(W):
                acc = COEFFS[j + 1] * E[t + 1, W - 1, ys, :]
                for i in range(j + 2, 5):
                    acc = acc + COEFFS[i] * E[t + 1, W + j - i, ys, :]
                target[base + j, ys, :] += cour[j, ys, :] * acc

        @pl.when(has_high)
        def _():
            halo(t, c, 0, False, W).wait_recv()
            for j in range(W):
                z = depth - 1 - j
                acc = COEFFS[j + 1] * E[t + 1, W + depth, ys, :]
                for i in range(j + 2, 5):
                    acc = acc + COEFFS[i] * E[t + 1, W + z + i, ys, :]
                target[base + z, ys, :] += cour[z, ys, :] * acc

    first_z = space * depth
    core = lax.rem(shot, 2)
    pair = shot // 2
    pairs = nshot // 2
    yq = rows // nshot
    pieces = (((W, inner),), ((0, W), (depth - W, W)))

    def quarter(index):
        return pl.ds(pl.multiple_of(index * yq, yq), yq)

    def mute(z):
        dz = first_z + z - source_s[0, 0]
        dy = lax.broadcasted_iota(jnp.int32, (rows, cols), 0) - source_s[0, 1]
        dx = lax.broadcasted_iota(jnp.int32, (rows, cols), 1) - source_s[0, 2]
        dist = (dz * dz + dy * dy + dx * dx).astype(F32)
        IM[z] = IM[z] * (1.0 - jnp.exp(dist * (-1.0 / (2.0 * MUTE * MUTE))))

    def copy_a(source, target, n):
        return pltpu.make_async_remote_copy(
            src_ref=source,
            dst_ref=target,
            send_sem=a_send.at[n],
            recv_sem=a_recv.at[n],
            device_id={"shot": shot + 1 - 2 * core},
            device_id_type=MESH,
        )

    def copy_b(d, n, at):
        other = lax.rem(pair + d, pairs)
        return pltpu.make_async_remote_copy(
            src_ref=S.at[other, at],
            dst_ref=RB.at[d - 1, at],
            send_sem=b_send.at[d - 1, n],
            recv_sem=b_recv.at[d - 1, n],
            device_id={"shot": 2 * other + core},
            device_id_type=MESH,
        )

    def whole_of(n):
        return pl.ds(0, sum(count for _, count in pieces[n]))

    def offer(n):
        for piece in pieces[n]:
            at = pl.ds(*piece)
            for h in range(pairs):
                copy_a(IM.at[at, quarter(2 * h + 1 - core), :], RA.at[h, at], n).start()

    def pass_on(n):
        copy_a(S.at[:, whole_of(n)], RA.at[:, whole_of(n)], n).wait()
        for piece in pieces[n]:
            at = pl.ds(*piece)
            for h in range(pairs):
                S[h, at] = IM[at, quarter(2 * h + core), :] + RA[h, at]
            for d in range(1, pairs):
                copy_b(d, n, at).start()

    @pl.loop(0, ITERS - 1)
    def _(t):
        fix(t, 0, E.at[t + 2], W)
        send(t + 1, 0)

        @pl.when(t == 1)
        def _():
            pair_copy().wait()

        @pl.when(t > 0)
        def _():
            chain(2 * t - 2)

        @pl.when(t < 2)
        def _():
            decode(2 * t)

        relay(t, 1)

        @pl.when(t < 2)
        def _():
            decode(2 * t + 1)

        @pl.when(t == ITERS - 2)
        def _():
            pass_on(0)

        fix(t, 1, E.at[t + 2], W)
        send(t + 1, 1)

        @pl.when(t == ITERS - 2)
        def _():
            for low in (0, depth - W):

                @pl.loop(low, low + W)
                def _(z):
                    IM[z] = IM[z] + E[ITERS, W + z] * D[ITERS - 2, z]
                    mute(z)

            offer(1)

        local(t + 1, groups[:2])
        relay(t + 1, 0)

        @pl.when(t == ITERS - 2)
        def _():
            pass_on(1)

        local(t + 1, groups[2:])

        @pl.when(t > 0)
        def _():
            chain(2 * t - 1)

        drain(t, 0)
        drain(t, 1)

        @pl.when(t == ITERS - 3)
        def _():
            @pl.loop(0, depth)
            def _(z):
                value = IM[z]
                for k in range(ITERS - 2):
                    value = value + E[k + 2, W + z] * D[k, z]
                IM[z] = value

            @pl.loop(W, depth - W)
            def _(z):
                IM[z] = IM[z] + E[ITERS, W + z] * D[ITERS - 2, z]
                mute(z)

            offer(0)

    @pl.loop(0, depth)
    def _(z):
        second[z] = E[ITERS, W + z]
        first[z] = E[ITERS + 1, W + z]

    fix(ITERS - 1, 0, first, 0)
    relay(ITERS - 1, 1)
    drain(ITERS - 1, 0)
    total = S[pair]
    for d in range(1, pairs):
        for n in range(len(pieces)):
            copy_b(d, n, whole_of(n)).wait()
        total = total + RB[d - 1]
    grad[...] = total

    whole = jnp.zeros((8, 128), F32)
    for way in (0, 1):
        @pl.when(column != (columns - 1 if way else 0))
        def _():
            chain_copy(way).wait_send()

    @pl.when(column < columns - 1)
    def _():
        CO[1] = CO[1] + CI[0]

    for k in range(columns):
        whole = whole + CO[1, k]
    misfit[...] = whole

    fix(ITERS - 1, 1, first, 0)

    drain(ITERS - 1, 1)


def finish(factor, grad, first, second, total, grad_o, first_o, second_o, misfit, sem):
    copies = [
        pltpu.make_async_copy(source, target, sem.at[n])
        for n, (source, target) in enumerate(((first, first_o), (second, second_o), (grad, grad_o)))
    ]
    for copy in copies:
        copy.start()
    misfit[...] = total[0:1, 0:1] * factor
    for copy in copies:
        copy.wait()


def body(
    nshot,
    nspace,
    adjoint_now,
    adjoint_later,
    courant,
    checkpoint_codes,
    scale_index,
    scale_table,
    receiver_cell,
    observed,
    source_cell,
):
    depth, rows, cols = courant.shape
    levels = checkpoint_codes.shape[1]
    nrec = receiver_cell.shape[1]
    blocks = cols // QBLOCK
    pairs = nshot // 2
    yq = rows // nshot
    vmem = pl.BlockSpec(memory_space=pltpu.VMEM)
    anyspace = pl.BlockSpec(memory_space=pltpu.HBM)
    dma = pltpu.SemaphoreType.DMA
    held = pltpu.VMEM((depth, rows, cols), F32)
    field = jax.ShapeDtypeStruct((depth, rows, cols), F32)
    columns = nspace // 2
    most = max(W * (columns - 1) // columns, 1)
    gradient, first, second, total = pl.pallas_call(
        functools.partial(kernel, nshot, nspace),
        out_shape=(
            pltpu.VMEM((depth, yq, cols), F32),
            held,
            held,
            pltpu.VMEM((8, 128), F32),
        ),
        in_specs=[anyspace] * 9,
        out_specs=(vmem, vmem, vmem, vmem),
        scratch_shapes=[
            pltpu.SMEM(receiver_cell.shape, jnp.int32),
            pltpu.SMEM(source_cell.shape, jnp.int32),
            pltpu.SMEM(scale_table.shape, F32),
            pltpu.SMEM(observed.shape[1:], F32),
            pltpu.VMEM(scale_index.shape[1:], jnp.int32),
            pltpu.VMEM(receiver_cell.shape, jnp.int32),
            pltpu.VMEM((ITERS + 2, depth + 2 * W, rows, cols), F32),
            pltpu.VMEM((ITERS - 1, depth, rows, cols), F32),
            pltpu.VMEM((depth, rows, cols), F32),
            pltpu.VMEM((levels, depth, rows, QBLOCK), jnp.int32),
            pltpu.VMEM((128 // depth, depth, rows * blocks), F32),
            pltpu.VMEM((blocks, rows, 128), F32),
            pltpu.VMEM((nrec, 128), jnp.int32),
            pltpu.VMEM((ITERS, nrec, 128), F32),
            pltpu.VMEM((depth, rows, cols), F32),
            pltpu.VMEM((pairs, depth, yq, cols), F32),
            pltpu.VMEM((pairs, depth, yq, cols), F32),
            pltpu.VMEM((max(pairs - 1, 1), depth, yq, cols), F32),
            pltpu.VMEM((depth, rows, nrec), BF16),
            pltpu.VMEM((ITERS, nrec, cols), BF16),
            pltpu.VMEM((ITERS, nrec, cols), BF16),
            pltpu.VMEM((cols, cols), BF16),
            pltpu.VMEM((cols, cols), BF16),
            pltpu.VMEM((ITERS, nrec, QBLOCK), jnp.int32),
            pltpu.VMEM((ITERS, nrec, rows * blocks), F32),
            pltpu.VMEM((nshot, 8, 128), F32),
            pltpu.VMEM((8, 128), F32),
            pltpu.VMEM((8, 128), F32),
            pltpu.VMEM((8, 128), F32),
            pltpu.VMEM((2, columns, 8, 128), F32),
            pltpu.VMEM((2, columns, 8, 128), F32),
            pltpu.VMEM((ITERS, NC, most, rows // NC, cols), F32),
            dma((2, 2, NC)),
            dma((2, 2, NC)),
            dma((2, NC, most)),
            dma((2, NC)),
            dma((2,)),
            dma((2,)),
            dma((max(pairs - 1, 1), 2)),
            dma((max(pairs - 1, 1), 2)),
            dma((2,)),
            dma((2,)),
            dma((2,)),
            dma((2,)),
            dma((6,)),
            dma((4 + NC,)),
            pltpu.SemaphoreType.REGULAR,
        ],
        compiler_params=pltpu.CompilerParams(
            collective_id=0, has_side_effects=True, vmem_limit_bytes=52000000
        ),
    )(
        receiver_cell,
        source_cell,
        scale_table,
        observed[0],
        adjoint_now[0],
        adjoint_later[0],
        courant,
        checkpoint_codes[0],
        scale_index[0],
    )
    count = nshot * ITERS * nrec * nspace
    gradient, first, second, misfit = pl.pallas_call(
        functools.partial(finish, 0.5 / count),
        out_shape=(jax.ShapeDtypeStruct(gradient.shape, F32), field, field, jax.ShapeDtypeStruct((1, 1), F32)),
        in_specs=[vmem] * 4,
        out_specs=(anyspace, anyspace, anyspace, vmem),
        scratch_shapes=[dma((3,))],
        compiler_params=pltpu.CompilerParams(vmem_limit_bytes=16000000),
    )(gradient, first, second, total)
    return (gradient, first[None], second[None], misfit.reshape(()))


def solution(mesh):
    placed = (
        P("shot", "space", None, None),
        P("shot", "space", None, None),
        P("space", None, None),
        P("shot", None, "space", None, None),
        P("shot", None, "space", None),
        P(),
        P("shot", "space"),
        P("shot", None, "space"),
        P("shot", None),
    )
    return jax.shard_map(
        functools.partial(body, mesh.shape["shot"], mesh.shape["space"]),
        mesh=mesh,
        in_specs=placed,
        out_specs=(
            P("space", "shot", None),
            P("shot", "space", None, None),
            P("shot", "space", None, None),
            P(),
        ),
        check_vma=False,
    )
```
